32 devices in a mesh: sp: 4 (over z), bn: 2 (over x), dp: 4 (over y, core).
Axes of the slice: x: 2, y: 2, z: 4, core: 2. Of those that a mesh axis runs over, the one named last changes fastest.
Arguments:
- images: bfloat16 [8, 4, 64, 40, 128], P(('bn', 'dp'), 'sp'), may hold values from -8 to 8, as said below
- out_grad: bfloat16 [8, 4, 256, 40, 128], P(('bn', 'dp'), 'sp'), may hold values from -8 to 8, as said below
- conv_weight: bfloat16 [3, 3, 64, 64], replicated, may hold values from -0.25 to 0.25
- proj_weight: bfloat16 [64, 256], replicated, may hold values from -0.75 to 0.75
- gain_one: float32 [64], replicated, may hold values from 0.1 to 1.9
- shift_one: float32 [64], replicated, may hold values from -3 to 3
- gain_three: float32 [256], replicated, may hold values from 0.1 to 1.9
- shift_three: float32 [256], replicated, may hold values from -3 to 3
Outputs:
- images_grad: bfloat16 [8, 4, 64, 40, 128], P(('bn', 'dp'), 'sp')
- conv_grad: float32 [3, 3, 64, 64], replicated
- proj_grad: float32 [64, 256], replicated
- gain_one_grad: float32 [64], replicated
- shift_one_grad: float32 [64], replicated
- gain_three_grad: float32 [256], replicated
- shift_three_grad: float32 [256], replicated
The draws below stay inside these ranges and needn't reach their ends.
Inputs may be any that keep to these rules, and one draw needn't show every extreme that they name: `images`: channels of one quadrant have their own offset and spread. `out_grad`: channels of one quadrant have their own offset and spread.
All inputs are finite; a program needn't handle non-finite values.
Results may differ from the reference program's by a relative error of at most 0.029.
Values may be sent and summed in bfloat16 or wider, within the bound.
No kernel may reach another device: no remote copies, remote signals or barrier semaphores. Data moves between devices by JAX's collectives and lax.ppermute only.
A program may use at most 64 MiB of HBM per device.

```python
import jax
import jax.numpy as jnp
from jax import lax

C = 64
CO = 256
TH = 40
TW = 128
IMG_DEV = 1
IMAGES = 8
N_BN = 2
N_DP = 4


def tile_draw(key, channels, salt_value):
    folded = jax.random.fold_in(key, salt_value)
    subkeys = jax.random.split(folded, 4)
    corner = (IMAGES, 4, channels, 1, 1)
    whole = (IMAGES, 4, channels, TH, TW)
    offsets = 1.5 * jax.random.normal(subkeys[0], corner, jnp.float32)
    spreads = jnp.exp(jax.random.uniform(subkeys[1], corner, jnp.float32, -1.2, 0.5))
    jitter = jax.random.normal(subkeys[2], whole, jnp.float32)
    drawn = offsets + spreads * jitter
    return jnp.clip(drawn, -8.0, 8.0)


def draw_images(key, part):
    return tile_draw(key, C, 3).astype(jnp.bfloat16)


def draw_out_grad(key, part):
    return tile_draw(key, CO, 7).astype(jnp.bfloat16)


def noise(stream_key, extent, scale, bound, held_as=jnp.bfloat16):
    return jnp.clip(scale * jax.random.normal(stream_key, extent, jnp.float32), -bound, bound).astype(held_as)


def setup_inputs(seed: int = 0) -> dict:
    key_of = jax.random.split(jax.random.key(seed), 9)
    return {
        "images": draw_images(jax.random.fold_in(key_of[8], 71), 0),
        "out_grad": draw_out_grad(jax.random.fold_in(key_of[8], 71), 0),
        "conv_weight": noise(key_of[2], (3, 3, C, C), (9 * C) ** -0.5, 0.25),
        "proj_weight": noise(key_of[3], (C, CO), C ** -0.5, 0.75),
        "gain_one": jnp.clip(1.0 + 0.18 * jax.random.normal(key_of[4], (C,), jnp.float32), 0.1, 1.9),
        "shift_one": noise(key_of[5], (C,), 1.0, 3.0, jnp.float32),
        "gain_three": jnp.clip(1.0 + 0.18 * jax.random.normal(key_of[6], (CO,), jnp.float32), 0.1, 1.9),
        "shift_three": noise(key_of[7], (CO,), 1.0, 3.0, jnp.float32),
    }


norm_floor = 1e-05

def silu_slope(inputs):
    sigma = jax.nn.sigmoid(inputs)
    return sigma * (1.0 + inputs * (1.0 - sigma))

def channel(vector):
    return vector[None, :, None, None]

def assemble(tiles):
    groups, quadrants, depth, tile_rows, tile_cols = tiles.shape
    merged = tiles.reshape(groups, 2, 2, depth, tile_rows, tile_cols)
    return merged.transpose(0, 3, 1, 4, 2, 5).reshape(groups, depth, 2 * tile_rows, 2 * tile_cols)

def split_back(field):
    groups, depth, height, breadth = field.shape
    parted = field.reshape(groups, depth, 2, height // 2, 2, breadth // 2)
    return parted.transpose(0, 2, 4, 1, 3, 5).reshape(groups, 4, depth, height // 2, breadth // 2)

def shifted(padded, start_row, start_col, height, breadth):
    return padded[:, :, start_row:start_row + height, start_col:start_col + breadth].astype(jnp.float32)

def pad_cells(field):
    return jnp.pad(field, ((0, 0), (0, 0), (1, 1), (1, 1)))

def moments(values):
    average = lax.optimization_barrier(jnp.mean(values, axis=(0, 2, 3)))
    centred = values - channel(average)
    return (average, lax.optimization_barrier(jnp.mean(centred * centred, axis=(0, 2, 3))))

def group_pass(image_tiles, cot_tiles, conv_weight, proj_weight, gain_one, shift_one, gain_three, shift_three):
    field = assemble(image_tiles)
    cotangent = assemble(cot_tiles)
    height = field.shape[2]
    breadth = field.shape[3]
    cell_count = field.shape[0] * height * breadth
    padded = pad_cells(field)
    kernel = conv_weight.astype(jnp.float32)
    conv_out = None
    for row_off in range(3):
        for col_off in range(3):
            partial_sum = jnp.einsum('oi,gihw->gohw', kernel[row_off, col_off], shifted(padded, row_off, col_off, height, breadth))
            conv_out = partial_sum if conv_out is None else conv_out + partial_sum
    mean_one, var_one = moments(conv_out)
    scale_one = lax.rsqrt(var_one + norm_floor)
    normed_one = (conv_out - channel(mean_one)) * channel(scale_one)
    before_act = channel(gain_one) * normed_one + channel(shift_one)
    hidden = jax.nn.silu(before_act).astype(jnp.bfloat16)
    hidden_float = hidden.astype(jnp.float32)
    project = proj_weight.astype(jnp.float32)
    widened = jnp.einsum('io,gihw->gohw', project, hidden_float)
    mean_three, var_three = moments(widened)
    scale_three = lax.rsqrt(var_three + norm_floor)
    normed_three = (widened - channel(mean_three)) * channel(scale_three)
    output_pre = channel(gain_three) * normed_three + channel(shift_three)
    grad_out = cotangent.astype(jnp.float32) * silu_slope(output_pre)
    sum_three = lax.optimization_barrier(jnp.sum(grad_out, axis=(0, 2, 3)))
    cross_three = lax.optimization_barrier(jnp.sum(grad_out * normed_three, axis=(0, 2, 3)))
    grad_wide = channel(gain_three * scale_three) * (grad_out - channel(sum_three) / cell_count - normed_three * channel(cross_three) / cell_count)
    grad_wide = grad_wide.astype(jnp.bfloat16).astype(jnp.float32)
    grad_proj = jnp.einsum('gihw,gohw->io', hidden_float, grad_wide)
    grad_hidden = jnp.einsum('io,gohw->gihw', project, grad_wide)
    grad_pre = grad_hidden * silu_slope(before_act)
    sum_one = lax.optimization_barrier(jnp.sum(grad_pre, axis=(0, 2, 3)))
    cross_one = lax.optimization_barrier(jnp.sum(grad_pre * normed_one, axis=(0, 2, 3)))
    grad_conv_out = channel(gain_one * scale_one) * (grad_pre - channel(sum_one) / cell_count - normed_one * channel(cross_one) / cell_count)
    grad_conv_out = grad_conv_out.astype(jnp.bfloat16)
    back_float = grad_conv_out.astype(jnp.float32)
    pieces_list = []
    for row_off in range(3):
        for col_off in range(3):
            pieces_list.append(jnp.einsum('gohw,gihw->oi', back_float, shifted(padded, row_off, col_off, height, breadth)))
    grad_kernel = jnp.stack(pieces_list).reshape(kernel.shape)
    back_pad = pad_cells(grad_conv_out)
    grad_field = None
    for row_off in range(3):
        for col_off in range(3):
            partial_sum = jnp.einsum('oi,gohw->gihw', kernel[row_off, col_off], shifted(back_pad, 2 - row_off, 2 - col_off, height, breadth))
            grad_field = partial_sum if grad_field is None else grad_field + partial_sum
    return (split_back(grad_field.astype(jnp.bfloat16)), grad_kernel, grad_proj, cross_one, sum_one, cross_three, sum_three)

def reference(images, out_grad, conv_weight, proj_weight, gain_one, shift_one, gain_three, shift_three):

    def regroup(tiles):
        depth = tiles.shape[2]
        sectioned = tiles.reshape(N_BN, N_DP, IMG_DEV, 4, depth, TH, TW).transpose(1, 0, 2, 3, 4, 5, 6)
        return sectioned.reshape(N_DP, N_BN * IMG_DEV, 4, depth, TH, TW)

    def one_group(inputs_pair):
        return group_pass(inputs_pair[0], inputs_pair[1], conv_weight, proj_weight, gain_one, shift_one, gain_three, shift_three)
    results = lax.map(one_group, (regroup(images), regroup(out_grad)))
    grad_tiles = results[0].reshape(N_DP, N_BN, IMG_DEV, 4, C, TH, TW).transpose(1, 0, 2, 3, 4, 5, 6)
    grad_tiles = grad_tiles.reshape(IMAGES, 4, C, TH, TW)
    per_image = 1.0 / (4 * TH * TW)
    return (grad_tiles, lax.optimization_barrier(jnp.sum(results[1], axis=0)) * per_image, lax.optimization_barrier(jnp.sum(results[2], axis=0)) * per_image, lax.optimization_barrier(jnp.sum(results[3], axis=0)) * per_image, lax.optimization_barrier(jnp.sum(results[4], axis=0)) * per_image, lax.optimization_barrier(jnp.sum(results[5], axis=0)) * per_image, lax.optimization_barrier(jnp.sum(results[6], axis=0)) * per_image)
```

```python
import jax
import jax.numpy as jnp
from jax import lax
from jax.experimental import pallas as pl
from jax.experimental.pallas import tpu as pltpu
from jax.sharding import PartitionSpec as P

norm_floor = 1e-05
bf16 = jnp.bfloat16
f32 = jnp.float32
group_axes = ("sp", "bn")
all_axes = ("sp", "bn", "dp")


def from_partner(value, mask):
    return lax.ppermute(value, "sp", [(i, i ^ mask) for i in range(lax.axis_size("sp"))])


def nt_dot(left, right):
    return lax.dot_general(left, right, (((1,), (1,)), ((), ())), preferred_element_type=f32)


def nn_dot(left, right):
    return lax.dot_general(left, right, (((1,), (0,)), ((), ())), preferred_element_type=f32)


def lane_pair(ref, row):
    return jnp.concatenate([ref[row], ref[row + 1]], axis=1)


def fold_pair(value):
    half = value.shape[1] // 2
    return value[:, :half] + value[:, half:]


def flip(block):
    return jnp.transpose(block)


def row_of(partials):
    depth = partials.shape[0]
    if depth < 128:
        partials = jnp.concatenate([partials, jnp.zeros((128 - depth, 128), f32)], axis=0)
    pieces = [
        jnp.sum(jnp.transpose(partials[k : k + 128]), axis=0, keepdims=True)
        for k in range(0, partials.shape[0], 128)
    ]
    return pieces[0] if len(pieces) == 1 else jnp.concatenate(pieces, axis=1)


def columns_of(rows, depth):
    width = rows[0].shape[1]
    stacked = jnp.concatenate(rows + [jnp.zeros((128 - len(rows), width), f32)], axis=0)
    pieces = [jnp.transpose(stacked[:, k : k + 128]) for k in range(0, width, 128)]
    tall = pieces[0] if len(pieces) == 1 else jnp.concatenate(pieces, axis=0)
    return [tall[:depth, k : k + 1] for k in range(len(rows))]


def pack_rows(out_ref, rows):
    width = out_ref.shape[1]
    out_ref[...] = jnp.concatenate(
        rows + [jnp.zeros((out_ref.shape[0] - len(rows), width), f32)], axis=0
    )


def joined_moments(gathered_ref, local_cells):
    devices = gathered_ref.shape[0]
    means = [gathered_ref[d, 0:1, :] for d in range(devices)]
    average = sum(means[1:], means[0]) * (1.0 / devices)
    squares = None
    for d in range(devices):
        delta = means[d] - average
        term = gathered_ref[d, 1:2, :] + local_cells * (delta * delta)
        squares = term if squares is None else squares + term
    return average, squares * (1.0 / (devices * local_cells))


def summed_rows(gathered_ref, row):
    devices = gathered_ref.shape[0]
    total = gathered_ref[0, row : row + 1, :]
    for d in range(1, devices):
        total = total + gathered_ref[d, row : row + 1, :]
    return total


def logistic(value):
    return 0.5 * jnp.tanh(0.5 * value) + 0.5


def three_shifts(source_ref, top_ref, bottom_ref, left_ref, right_ref, out_ref):
    rows = source_ref.shape[0]
    depth, cols = top_ref.shape
    lane = lax.broadcasted_iota(jnp.int32, (depth, cols), 1)
    left = left_ref[...].astype(f32)
    right = right_ref[...].astype(f32)

    def place(r, line):
        before = pltpu.roll(line, 1, 1)
        after = pltpu.roll(line, cols - 1, 1)
        edge_left = pltpu.roll(left, (cols - r) % cols, 1)
        edge_right = pltpu.roll(right, (2 * cols - 1 - r) % cols, 1)
        before = jnp.where(lane == 0, edge_left, before)
        after = jnp.where(lane == cols - 1, edge_right, after)
        out_ref[r] = jnp.concatenate([before, line, after], axis=0).astype(bf16)

    place(0, top_ref[...].astype(f32))
    place(rows + 1, bottom_ref[...].astype(f32))

    def body(h, carry):
        place(h + 1, source_ref[h].astype(f32))
        return carry

    lax.fori_loop(0, rows, body, 0, unroll=2)


def conv_pair(weights, shifted_ref, row):
    depth3 = shifted_ref.shape[1]
    cols = shifted_ref.shape[2]
    first = shifted_ref[pl.ds(row, 3)].reshape(3 * depth3, cols)
    second = shifted_ref[pl.ds(row + 1, 3)].reshape(3 * depth3, cols)
    return nn_dot(weights, jnp.concatenate([first, second], axis=1))


def conv_kernel(x_ref, top_ref, bottom_ref, left_ref, right_ref, w_ref, shifted_ref, a_ref, stat_ref):
    rows, depth, cols = x_ref.shape
    three_shifts(x_ref, top_ref, bottom_ref, left_ref, right_ref, shifted_ref)
    weights = w_ref[...]

    def body(j, total):
        h = 2 * j
        both = conv_pair(weights, shifted_ref, h)
        a_ref[h] = both[:, :cols]
        a_ref[h + 1] = both[:, cols:]
        return total + fold_pair(both)

    total = lax.fori_loop(0, rows // 2, body, jnp.zeros((depth, cols), f32))
    mean = jnp.sum(total, axis=1, keepdims=True) * (1.0 / (rows * cols))

    def spread(h, squares):
        centred = a_ref[h] - mean
        return squares + centred * centred

    squares = lax.fori_loop(0, rows, spread, jnp.zeros((depth, cols), f32), unroll=4)
    pack_rows(stat_ref, [row_of(total) * (1.0 / (rows * cols)), row_of(squares)])


def first_norm(gathered_ref, par_ref, local_cells, depth):
    average, variance = joined_moments(gathered_ref, local_cells)
    scale = lax.rsqrt(variance + norm_floor)
    mean, scale = columns_of([average, scale], depth)
    return mean, scale, par_ref[:, 0:1], par_ref[:, 1:2]


def hidden_kernel(a_ref, stat_ref, par_ref, w_ref, y_ref, out_ref):
    rows, depth, cols = a_ref.shape
    wide = w_ref.shape[0]
    mean, scale, gain, shift = first_norm(stat_ref, par_ref, float(rows * cols), depth)
    steep = gain * scale

    def activate(h, total):
        before = (a_ref[h] - mean) * steep + shift
        hidden = (before * logistic(before)).astype(bf16)
        y_ref[h] = hidden
        return total + hidden.astype(f32)

    total = lax.fori_loop(0, rows, activate, jnp.zeros((depth, cols), f32), unroll=2)
    weights = w_ref[...]
    mean_y = row_of(total)[:, :depth] * (1.0 / (rows * cols))
    mean_b = jnp.sum(weights.astype(f32) * mean_y, axis=1, keepdims=True)

    def spread(j, squares):
        widened = nn_dot(weights, lane_pair(y_ref, 2 * j)) - mean_b
        return squares + fold_pair(widened * widened)

    squares = lax.fori_loop(0, rows // 2, spread, jnp.zeros((wide, cols), f32))
    lane = lax.broadcasted_iota(jnp.int32, (wide, cols), 1)
    mean_row = row_of(jnp.where(lane == 0, mean_b, 0.0))
    pack_rows(out_ref, [mean_row, row_of(squares)])


def third_norm(gathered_ref, par_ref, local_cells, wide):
    average, variance = joined_moments(gathered_ref, local_cells)
    scale = lax.rsqrt(variance + norm_floor)
    mean, scale = columns_of([average, scale], wide)
    return mean, scale, par_ref[:, 0:1], par_ref[:, 1:2]


def slope_kernel(y_ref, g_ref, stat_ref, par_ref, w_ref, e_ref, out_ref):
    rows, depth, cols = y_ref.shape
    wide = w_ref.shape[0]
    mean, scale, gain, shift = third_norm(stat_ref, par_ref, float(rows * cols), wide)
    weights = w_ref[...]

    def body(j, carry):
        total, cross = carry
        h = 2 * j
        widened = nn_dot(weights, lane_pair(y_ref, h))
        normed = (widened - mean) * scale
        before = gain * normed + shift
        sigma = logistic(before)
        act = before * sigma
        slope = sigma + act * (1.0 - sigma)
        grad = lane_pair(g_ref, h).astype(f32) * slope
        e_ref[h] = grad[:, :cols].astype(bf16)
        e_ref[h + 1] = grad[:, cols:].astype(bf16)
        return total + fold_pair(grad), cross + fold_pair(grad * normed)

    zero = jnp.zeros((wide, cols), f32)
    total, cross = lax.fori_loop(0, rows // 2, body, (zero, zero))
    pack_rows(out_ref, [row_of(total), row_of(cross)])


def wide_kernel(
    y_ref, e_ref, a_ref, stat1_ref, par1_ref, stat3_ref, par3_ref, sums_ref, w_ref, wt_ref,
    e1_ref, out_ref, proj_ref,
):
    rows, depth, cols = y_ref.shape
    wide = w_ref.shape[0]
    local_cells = float(rows * cols)
    cells = local_cells * sums_ref.shape[0]
    mean3, scale3, gain3, _ = third_norm(stat3_ref, par3_ref, local_cells, wide)
    mean1, scale1, gain1, shift1 = first_norm(stat1_ref, par1_ref, local_cells, depth)
    total3, cross3 = columns_of([summed_rows(sums_ref, 0), summed_rows(sums_ref, 1)], wide)
    front = gain3 * scale3
    flat = total3 * (1.0 / cells)
    tilt = cross3 * (1.0 / cells)
    weights = w_ref[...]
    weights_t = wt_ref[...]

    def body(j, carry):
        total, cross, proj = carry
        h = 2 * j
        hidden = lane_pair(y_ref, h)
        normed = (nn_dot(weights, hidden) - mean3) * scale3
        grad_wide = front * (lane_pair(e_ref, h).astype(f32) - flat - normed * tilt)
        grad_wide = grad_wide.astype(bf16)
        proj = proj + nt_dot(grad_wide, hidden)
        normed1 = (lane_pair(a_ref, h) - mean1) * scale1
        before = gain1 * normed1 + shift1
        sigma = logistic(before)
        act = before * sigma
        grad = nn_dot(weights_t, grad_wide) * (sigma + act * (1.0 - sigma))
        e1_ref[h] = grad[:, :cols]
        e1_ref[h + 1] = grad[:, cols:]
        return total + fold_pair(grad), cross + fold_pair(grad * normed1), proj

    zero = jnp.zeros((depth, cols), f32)
    total, cross, proj = lax.fori_loop(
        0, rows // 2, body, (zero, zero, jnp.zeros((wide, depth), f32))
    )
    pack_rows(out_ref, [row_of(total), row_of(cross)])
    proj_ref[...] = proj


def kernel_grad_kernel(
    e1_ref, a_ref, shifted_ref, stat1_ref, par1_ref, sums_ref, da_ref, grad_ref, padded_ref
):
    rows, depth, cols = a_ref.shape
    local_cells = float(rows * cols)
    cells = local_cells * sums_ref.shape[0]
    mean1, scale1, gain1, _ = first_norm(stat1_ref, par1_ref, local_cells, depth)
    total1, cross1 = columns_of([summed_rows(sums_ref, 0), summed_rows(sums_ref, 1)], depth)
    front = gain1 * scale1
    flat = total1 * (1.0 / cells)
    tilt = cross1 * (1.0 / cells)
    blank = jnp.zeros((2, depth, cols), bf16)
    padded_ref[pl.ds(0, 2)] = blank
    padded_ref[pl.ds(rows + 2, 2)] = blank

    def back(h, carry):
        normed = (a_ref[h] - mean1) * scale1
        grad = (front * (e1_ref[h] - flat - normed * tilt)).astype(bf16)
        da_ref[h] = grad
        padded_ref[h + 2] = grad
        return carry

    lax.fori_loop(0, rows, back, 0, unroll=2)

    def gather(j, total):
        r = 2 * j
        first = padded_ref[pl.ds(r, 3)].reshape(3 * depth, cols)
        second = padded_ref[pl.ds(r + 1, 3)].reshape(3 * depth, cols)
        left = jnp.concatenate([first, second], axis=1)
        return total + nt_dot(left, lane_pair(shifted_ref, r))

    grad_ref[...] = lax.fori_loop(
        0, (rows + 2) // 2, gather, jnp.zeros((3 * depth, 3 * depth), f32)
    )


def back_kernel(d_ref, top_ref, bottom_ref, left_ref, right_ref, w_ref, out_ref, shifted_ref):
    rows, depth, cols = d_ref.shape
    three_shifts(d_ref, top_ref, bottom_ref, left_ref, right_ref, shifted_ref)
    weights = w_ref[...]

    def body(j, carry):
        h = 2 * j
        both = conv_pair(weights, shifted_ref, h).astype(bf16)
        out_ref[h] = both[:, :cols]
        out_ref[h + 1] = both[:, cols:]
        return carry

    lax.fori_loop(0, rows // 2, body, 0)


def call(kernel, outs, *args, scratch=()):
    return pl.pallas_call(
        kernel,
        out_shape=[jax.ShapeDtypeStruct(s, d) for s, d in outs],
        scratch_shapes=list(scratch),
        compiler_params=pltpu.CompilerParams(vmem_limit_bytes=56 * 1024 * 1024),
        name=kernel.__name__,
    )(*args)


def halo(lines):
    rows, depth, cols = lines.shape
    position = lax.axis_index("sp")
    column = position % 2
    half = position // 2
    edge_col = jnp.where(column == 0, lines[:, :, cols - 1], lines[:, :, 0])
    edge_row = jnp.where(half == 0, lines[rows - 1], lines[0])
    corner = jnp.where(half == 0, edge_col[rows - 1 : rows], edge_col[:1])
    got_col = from_partner(edge_col, 1)
    got_row = from_partner(edge_row, 2)
    got_corner = from_partner(corner, 3)
    none = jnp.zeros_like(got_row)
    top = jnp.where(half == 1, got_row, none)
    bottom = jnp.where(half == 0, got_row, none)
    blank = jnp.zeros_like(got_corner)
    side = jnp.concatenate(
        [jnp.where(half == 1, got_corner, blank), got_col, jnp.where(half == 0, got_corner, blank)],
        axis=0,
    )
    side = jnp.pad(side, ((0, cols - rows - 2), (0, 0))).T
    left = jnp.where(column == 1, side, jnp.zeros_like(side))
    right = jnp.where(column == 0, side, jnp.zeros_like(side))
    return top, bottom, left, right


def everyone(value, axes):
    count = lax.axis_size(axes)
    return lax.all_to_all(jnp.broadcast_to(value[None], (count,) + value.shape), axes, 0, 0)


def shards(
    images, out_grad, conv_weight, proj_weight, gain_one, shift_one, gain_three, shift_three
):
    depth, rows, cols = images.shape[2:]
    wide = out_grad.shape[2]
    group = lax.axis_size(group_axes)
    devices = lax.axis_size(all_axes)
    per_image = 1.0 / float(lax.axis_size("sp") * rows * cols)
    lines = jnp.transpose(images[0, 0], (1, 0, 2))
    cotangent = jnp.transpose(out_grad[0, 0], (1, 0, 2))
    ahead = jnp.transpose(conv_weight, (2, 0, 1, 3)).reshape(depth, 9 * depth)
    behind = jnp.transpose(conv_weight[::-1, ::-1], (3, 0, 1, 2)).reshape(depth, 9 * depth)
    proj_t = proj_weight.T
    par_one = jnp.stack([gain_one, shift_one], axis=1)
    par_three = jnp.stack([gain_three, shift_three], axis=1)
    wide_row = max(depth, 128)

    shifted, conv_out, stat = call(
        conv_kernel,
        [((rows + 2, 3 * depth, cols), bf16), ((rows, depth, cols), f32), ((8, wide_row), f32)],
        lines, *halo(lines), ahead,
    )
    stat_one = everyone(stat, group_axes)
    hidden, stat = call(
        hidden_kernel,
        [((rows, depth, cols), bf16), ((8, wide), f32)],
        conv_out, stat_one, par_one, proj_t,
    )
    stat_three = everyone(stat, group_axes)
    grad_out, sums = call(
        slope_kernel,
        [((rows, wide, cols), bf16), ((8, wide), f32)],
        hidden, cotangent, stat_three, par_three, proj_t,
    )
    sums_three = everyone(sums, group_axes)
    grad_pre, sums, proj = call(
        wide_kernel,
        [((rows, depth, cols), f32), ((8, wide_row), f32), ((wide, depth), f32)],
        hidden, grad_out, conv_out, stat_one, par_one, stat_three, par_three, sums_three,
        proj_t, proj_weight,
    )
    sums_one = everyone(sums, group_axes)
    grad_conv, kernel_part = call(
        kernel_grad_kernel,
        [((rows, depth, cols), bf16), ((3 * depth, 3 * depth), f32)],
        grad_pre, conv_out, shifted, stat_one, par_one, sums_one,
        scratch=[pltpu.VMEM((rows + 4, depth, cols), bf16)],
    )
    (grad_field,) = call(
        back_kernel,
        [((rows, depth, cols), bf16)],
        grad_conv, *halo(grad_conv), behind,
        scratch=[pltpu.VMEM((rows + 2, 3 * depth, cols), bf16)],
    )

    share = 1.0 / group
    small = jnp.concatenate(
        [
            jnp.sum(sums_one[:, 1, :depth], axis=0), jnp.sum(sums_one[:, 0, :depth], axis=0),
            jnp.sum(sums_three[:, 1], axis=0), jnp.sum(sums_three[:, 0], axis=0),
        ]
    ) * share
    small_high = small.astype(bf16)
    small_low = (small - small_high.astype(f32)).astype(bf16)
    flat = jnp.concatenate(
        [kernel_part.astype(bf16).reshape(-1), proj.astype(bf16).reshape(-1), small_high, small_low]
    )
    used = flat.shape[0]
    unit = devices * 16 * 128
    flat = jnp.pad(flat, (0, -used % unit)).reshape(devices, -1, 128)
    parts = lax.all_to_all(flat, all_axes, 0, 0)
    mine = jnp.sum(parts.astype(f32), axis=0).astype(bf16)
    full = everyone(mine, all_axes).reshape(-1).astype(f32) * per_image
    cut = 9 * depth * depth
    kernel_total = full[:cut].reshape(3, depth, 3, depth)[::-1].transpose(0, 2, 1, 3)
    proj_total = full[cut : cut + wide * depth].reshape(wide, depth).T
    tail = cut + wide * depth
    count = 2 * depth + 2 * wide
    small = full[tail : tail + count] + full[tail + count : tail + 2 * count]
    return (
        jnp.transpose(grad_field, (1, 0, 2))[None, None],
        kernel_total,
        proj_total,
        small[:depth],
        small[depth : 2 * depth],
        small[2 * depth : 2 * depth + wide],
        small[2 * depth + wide :],
    )


def solution(mesh):
    in_specs = (
        P(("bn", "dp"), "sp", None, None, None),
        P(("bn", "dp"), "sp", None, None, None),
        P(),
        P(),
        P(),
        P(),
        P(),
        P(),
    )
    out_specs = (P(("bn", "dp"), "sp", None, None, None), P(), P(), P(), P(), P(), P())
    return jax.shard_map(shards, mesh=mesh, in_specs=in_specs, out_specs=out_specs, check_vma=False)
```

```python
from functools import partial

import jax
import jax.numpy as jnp
from jax import lax
from jax.experimental import pallas as pl
from jax.experimental.pallas import tpu as pltpu
from jax.sharding import PartitionSpec as P

norm_floor = 1e-05
bf16 = jnp.bfloat16
f32 = jnp.float32
EDGE, LINES, CONV, HIDDEN, SLOPE, WIDE, GRAD, PACK, BACK = 8, 16, 12, 12, 16, 24, 16, 4, 12
group_axes = ("sp", "bn")
all_axes = ("sp", "bn", "dp")


def from_partner(value, mask):
    return lax.ppermute(value, "sp", [(i, i ^ mask) for i in range(lax.axis_size("sp"))])


def nt_dot(left, right):
    return lax.dot_general(left, right, (((1,), (1,)), ((), ())), preferred_element_type=f32)


def nn_dot(left, right):
    return lax.dot_general(left, right, (((1,), (0,)), ((), ())), preferred_element_type=f32)


def lane_pair(ref, row):
    return jnp.concatenate([ref[row], ref[row + 1]], axis=1)


def fold_pair(value):
    half = value.shape[1] // 2
    return value[:, :half] + value[:, half:]


def flip(block):
    return jnp.transpose(block)


def row_of(partials):
    depth = partials.shape[0]
    if depth < 128:
        partials = jnp.concatenate([partials, jnp.zeros((128 - depth, 128), f32)], axis=0)
    pieces = [
        jnp.sum(jnp.transpose(partials[k : k + 128]), axis=0, keepdims=True)
        for k in range(0, partials.shape[0], 128)
    ]
    return pieces[0] if len(pieces) == 1 else jnp.concatenate(pieces, axis=1)


def columns_of(rows, depth):
    width = rows[0].shape[1]
    stacked = jnp.concatenate(rows + [jnp.zeros((128 - len(rows), width), f32)], axis=0)
    pieces = [jnp.transpose(stacked[:, k : k + 128]) for k in range(0, width, 128)]
    tall = pieces[0] if len(pieces) == 1 else jnp.concatenate(pieces, axis=0)
    return [tall[:depth, k : k + 1] for k in range(len(rows))]


def pack_rows(out_ref, rows):
    devices, height, width = out_ref.shape
    block = jnp.concatenate(rows + [jnp.zeros((height - len(rows), width), f32)], axis=0)
    for d in range(devices):
        out_ref[d] = block


def joined_moments(gathered_ref, local_cells):
    devices = gathered_ref.shape[0]
    means = [gathered_ref[d, 0:1, :] for d in range(devices)]
    average = sum(means[1:], means[0]) * (1.0 / devices)
    squares = None
    for d in range(devices):
        delta = means[d] - average
        term = gathered_ref[d, 1:2, :] + local_cells * (delta * delta)
        squares = term if squares is None else squares + term
    return average, squares * (1.0 / (devices * local_cells))


def summed_rows(gathered_ref, row):
    devices = gathered_ref.shape[0]
    total = gathered_ref[0, row : row + 1, :]
    for d in range(1, devices):
        total = total + gathered_ref[d, row : row + 1, :]
    return total


def logistic(value):
    return 0.5 * jnp.tanh(0.5 * value) + 0.5


def place_flags():
    position = lax.axis_index("sp")
    return position % 2, position // 2


def edge_pieces(line_of, rows, shape, row_ref, col_ref, corner_ref, at=0):
    depth, cols = shape
    column, half = place_flags()
    lane = lax.broadcasted_iota(jnp.int32, (depth, cols), 1)
    edge = jnp.where(column == 0, cols - 1, 0)

    def body(h, found):
        moved = pltpu.roll(line_of(h), lax.rem(h + 1 - edge + cols, cols), 1)
        return jnp.where(lane == h + 1, moved, found)

    kind = row_ref.dtype
    block = pl.ds(at, depth)
    found = lax.fori_loop(0, rows, body, jnp.zeros((depth, cols), f32), unroll=4)
    col_ref[block] = found.astype(kind)
    border = line_of(jnp.where(half == 0, rows - 1, 0))
    row_ref[block] = border.astype(kind)
    target = jnp.where(half == 0, 0, rows + 1)
    moved = pltpu.roll(border, lax.rem(target - edge + cols, cols), 1)
    corner_ref[block] = jnp.where(lane == target, moved, 0.0).astype(kind)


def three_shifts(line_of, border, side, out_ref):
    rows = out_ref.shape[0] - 2
    depth, cols = border.shape
    column, half = place_flags()
    lane = lax.broadcasted_iota(jnp.int32, (depth, cols), 1)
    left = jnp.where(column == 1, side, 0.0)
    right = jnp.where(column == 0, side, 0.0)

    def place(r, line):
        before = pltpu.roll(line, 1, 1)
        after = pltpu.roll(line, cols - 1, 1)
        edge_left = pltpu.roll(left, (cols - r) % cols, 1)
        edge_right = pltpu.roll(right, (2 * cols - 1 - r) % cols, 1)
        before = jnp.where(lane == 0, edge_left, before)
        after = jnp.where(lane == cols - 1, edge_right, after)
        out_ref[r] = jnp.concatenate([before, line, after], axis=0).astype(bf16)

    place(0, jnp.where(half == 1, border, 0.0))
    place(rows + 1, jnp.where(half == 0, border, 0.0))

    def body(h, carry):
        place(h + 1, line_of(h))
        return carry

    lax.fori_loop(0, rows, body, 0, unroll=4)


def conv_pair(weights, shifted_ref, row):
    depth3 = shifted_ref.shape[1]
    cols = shifted_ref.shape[2]
    first = shifted_ref[pl.ds(row, 3)].reshape(3 * depth3, cols)
    second = shifted_ref[pl.ds(row + 1, 3)].reshape(3 * depth3, cols)
    return nn_dot(weights, jnp.concatenate([first, second], axis=1))


def to_lines(planes_ref, out_ref, tall_ref):
    depth, rows, cols = planes_ref.shape
    block = tall_ref.shape[0] // rows
    for start in range(0, depth, block):

        def spill(c, carry, start=start):
            at = pl.multiple_of(c * rows, 8)
            tall_ref[pl.ds(at, rows), :] = planes_ref[start + c].astype(f32)
            return carry

        lax.fori_loop(0, block, spill, 0, unroll=8)

        def collect(h, carry, start=start):
            line = tall_ref[pl.ds(h, block, stride=rows), :]
            out_ref[h, start : start + block] = line.astype(bf16)
            return carry

        lax.fori_loop(0, rows, collect, 0, unroll=4)


def edge_kernel(planes_ref, lines_ref, row_ref, col_ref, corner_ref, tall_ref):
    rows, depth, cols = lines_ref.shape
    to_lines(planes_ref, lines_ref, tall_ref)
    edge_pieces(
        lambda h: lines_ref[h].astype(f32), rows, (depth, cols), row_ref, col_ref, corner_ref
    )


def lines_kernel(planes_ref, lines_ref, tall_ref):
    to_lines(planes_ref, lines_ref, tall_ref)


def conv_kernel(x_ref, row_ref, col_ref, corner_ref, w_ref, shifted_ref, a_ref, stat_ref):
    rows, depth, cols = x_ref.shape
    side = col_ref[...].astype(f32) + corner_ref[...].astype(f32)
    three_shifts(lambda h: x_ref[h].astype(f32), row_ref[...].astype(f32), side, shifted_ref)
    weights = w_ref[...]

    def body(j, total):
        h = 2 * j
        both = conv_pair(weights, shifted_ref, h)
        a_ref[h] = both[:, :cols]
        a_ref[h + 1] = both[:, cols:]
        return total + fold_pair(both)

    total = lax.fori_loop(0, rows // 2, body, jnp.zeros((depth, cols), f32), unroll=4)
    mean = jnp.sum(total, axis=1, keepdims=True) * (1.0 / (rows * cols))

    def spread(h, squares):
        centred = a_ref[h] - mean
        return squares + centred * centred

    squares = lax.fori_loop(0, rows, spread, jnp.zeros((depth, cols), f32), unroll=4)
    pack_rows(stat_ref, [row_of(total) * (1.0 / (rows * cols)), row_of(squares)])


def first_norm(gathered_ref, par_ref, local_cells, depth):
    average, variance = joined_moments(gathered_ref, local_cells)
    scale = lax.rsqrt(variance + norm_floor)
    mean, scale = columns_of([average, scale], depth)
    return mean, scale, par_ref[:, 0:1], par_ref[:, 1:2]


def spread_column(column, cols):
    return jnp.broadcast_to(column, (column.shape[0], cols))


def hidden_kernel(a_ref, stat_ref, par_ref, w_ref, y_ref, out_ref, centred_ref):
    rows, depth, cols = a_ref.shape
    cells = float(rows * cols)
    mean, scale, gain, shift = first_norm(stat_ref, par_ref, cells, depth)
    steep = spread_column(0.5 * gain * scale, cols)
    mean = spread_column(mean, cols)
    lift = spread_column(0.5 * shift, cols)
    middle = spread_column(shift * logistic(shift), cols).astype(bf16).astype(f32)

    def activate(h, total):
        half = (a_ref[h] - mean) * steep + lift
        hidden = (half + half * jnp.tanh(half)).astype(bf16)
        y_ref[h] = hidden
        centred = hidden.astype(f32) - middle
        centred_ref[h] = centred.astype(bf16)
        return total + centred

    total = lax.fori_loop(0, rows, activate, jnp.zeros((depth, cols), f32), unroll=4)
    gram = jnp.zeros((depth, depth), f32)
    step = 8
    for h in range(0, rows, step):
        wide_lines = jnp.concatenate([centred_ref[k] for k in range(h, min(h + step, rows))], axis=1)
        gram = gram + nt_dot(wide_lines, wide_lines)
    weights = w_ref[...].astype(f32)
    mean_c = jnp.sum(total, axis=1, keepdims=True) * (1.0 / cells)
    mean_r = row_of(total)[:, :depth] * (1.0 / cells)
    spread = gram - cells * (mean_c * mean_r)
    mixed = lax.dot_general(
        spread, weights, (((1,), (0,)), ((), ())),
        precision=lax.Precision.HIGHEST, preferred_element_type=f32,
    )
    squares = jnp.maximum(jnp.sum(mixed * weights, axis=0, keepdims=True), 0.0)
    means = jnp.sum(weights * (mean_c + middle[:, 0:1]), axis=0, keepdims=True)
    pack_rows(out_ref, [means, squares])


def third_norm(gathered_ref, par_ref, local_cells, wide):
    average, variance = joined_moments(gathered_ref, local_cells)
    scale = lax.rsqrt(variance + norm_floor)
    mean, scale = columns_of([average, scale], wide)
    return mean, scale, par_ref[:, 0:1], par_ref[:, 1:2]


def slope_kernel(y_ref, g_ref, stat_ref, par_ref, w_ref, e_ref, out_ref, keep_ref):
    rows, depth, cols = y_ref.shape
    wide = w_ref.shape[0]
    mean, scale, gain, shift = third_norm(stat_ref, par_ref, float(rows * cols), wide)
    steep = 0.5 * gain * scale
    keep_ref[0] = spread_column(mean, cols)
    keep_ref[1] = spread_column(steep, cols)
    keep_ref[2] = spread_column(0.5 * shift, cols)
    keep_ref[3] = jnp.zeros((wide, cols), f32)
    keep_ref[4] = jnp.zeros((wide, cols), f32)
    block = 128

    def body(j, carry):
        h = 2 * j
        lines = lane_pair(y_ref, h)
        for start in range(0, wide, block):
            part = slice(start, start + block)
            both = nn_dot(w_ref[part], lines)
            m, s, b = keep_ref[0, part], keep_ref[1, part], keep_ref[2, part]
            total = cross = None
            for k in range(2):
                half = (both[:, k * cols : (k + 1) * cols] - m) * s + b
                t = jnp.tanh(half)
                slope = (1.0 + t) * (1.0 + half * (1.0 - t))
                grad = g_ref[h + k, part].astype(f32) * slope
                e_ref[h + k, part] = grad.astype(bf16)
                across = grad * half
                total = grad if total is None else total + grad
                cross = across if cross is None else cross + across
            keep_ref[3, part] += total
            keep_ref[4, part] += cross
        return carry

    lax.fori_loop(0, rows // 2, body, 0, unroll=2)
    total = row_of(keep_ref[3]) * 0.5
    cross = row_of(keep_ref[4])
    lane_shift, lane_gain = row_of_column(shift, cols), row_of_column(gain, cols)
    pack_rows(out_ref, [total, (cross - lane_shift * total) / lane_gain])


def row_of_column(column, cols):
    lane = lax.broadcasted_iota(jnp.int32, (column.shape[0], cols), 1)
    return row_of(jnp.where(lane == 0, column, 0.0))


def wide_kernel(
    y_ref, e_ref, a_ref, stat1_ref, par1_ref, stat3_ref, par3_ref, sums_ref, w_ref, wt_ref,
    e1_ref, n1_ref, out_ref, proj_ref, row_ref, col_ref, corner_ref, keep_ref,
):
    rows, depth, cols = y_ref.shape
    wide = w_ref.shape[0]
    local_cells = float(rows * cols)
    cells = local_cells * sums_ref.shape[0]
    mean3, scale3, gain3, _ = third_norm(stat3_ref, par3_ref, local_cells, wide)
    mean1, scale1, gain1, shift1 = first_norm(stat1_ref, par1_ref, local_cells, depth)
    total3, cross3 = columns_of([summed_rows(sums_ref, 0), summed_rows(sums_ref, 1)], wide)
    front = gain3 * scale3
    tilt = front * scale3 * cross3 * (1.0 / cells)
    keep_ref[0] = spread_column(0.5 * front, cols)
    keep_ref[1] = spread_column(tilt, cols)
    keep_ref[2] = spread_column(front * total3 * (1.0 / cells) - tilt * mean3, cols)
    mean1 = spread_column(mean1, cols)
    scale1 = spread_column(scale1, cols)
    gain1 = spread_column(0.5 * gain1, cols)
    shift1 = spread_column(0.5 * shift1, cols)
    weights_t = wt_ref[...]
    block = 128

    def body(j, carry):
        total, cross, proj = carry
        h = 2 * j
        hidden = lane_pair(y_ref, h)
        pieces = []
        for start in range(0, wide, block):
            part = slice(start, start + block)
            both = nn_dot(w_ref[part], hidden)
            p, q, r = keep_ref[0, part], keep_ref[1, part], keep_ref[2, part]
            pieces.append(
                jnp.concatenate(
                    [
                        (p * e_ref[h + k, part].astype(f32) - q * both[:, k * cols : (k + 1) * cols] - r)
                        .astype(bf16)
                        for k in range(2)
                    ],
                    axis=1,
                )
            )
        grad_wide = jnp.concatenate(pieces, axis=0)
        proj = proj + nt_dot(hidden, grad_wide)
        back = nn_dot(weights_t, grad_wide)
        for k in range(2):
            normed = (a_ref[h + k] - mean1) * scale1
            half = gain1 * normed + shift1
            t = jnp.tanh(half)
            slope = (0.5 + 0.5 * t) * (1.0 + half * (1.0 - t))
            grad = back[:, k * cols : (k + 1) * cols] * slope
            e1_ref[h + k] = grad
            n1_ref[h + k] = normed
            total = total + grad
            cross = cross + grad * normed
        return total, cross, proj

    zero = jnp.zeros((depth, cols), f32)
    total, cross, proj = lax.fori_loop(
        0, rows // 2, body, (zero, zero, jnp.zeros((depth, wide), f32)), unroll=2
    )
    pack_rows(out_ref, [row_of(total), row_of(cross)])
    proj_ref[...] = proj
    edge_pieces(lambda h: e1_ref[h], rows, (depth, cols), row_ref, col_ref, corner_ref, 0)
    edge_pieces(lambda h: n1_ref[h], rows, (depth, cols), row_ref, col_ref, corner_ref, depth)


def corr_kernel(e1_ref, n1_ref, shifted_ref, out_ref, padded_ref):
    rows, depth, cols = e1_ref.shape
    tall = padded_ref.shape[1]
    blank = jnp.zeros((2, tall, cols), bf16)
    padded_ref[pl.ds(0, 2)] = blank
    padded_ref[pl.ds(rows + 2, 2)] = blank
    ones = jnp.ones((tall - 2 * depth, cols), bf16)

    def fill(h, carry):
        padded_ref[h + 2] = jnp.concatenate(
            [e1_ref[h].astype(bf16), n1_ref[h].astype(bf16), ones], axis=0
        )
        return carry

    lax.fori_loop(0, rows, fill, 0, unroll=4)
    step = 6
    total = jnp.zeros(out_ref.shape, f32)
    out_ref[...] = total
    for start in range(0, rows + 2, step):
        lines = range(start, min(start + step, rows + 2))
        left = jnp.concatenate(
            [padded_ref[pl.ds(r, 3)].reshape(3 * tall, cols) for r in lines], axis=1
        )
        right = jnp.concatenate([shifted_ref[r] for r in lines], axis=1)
        out_ref[...] += nt_dot(left, right)


def first_backward(stat1_ref, par1_ref, sums1_ref, local_cells, depth):
    cells = local_cells * sums1_ref.shape[0]
    _, scale1, gain1, _ = first_norm(stat1_ref, par1_ref, local_cells, depth)
    sums_one = [summed_rows(sums1_ref, 0), summed_rows(sums1_ref, 1)]
    total1, cross1 = columns_of(sums_one, depth)
    return gain1 * scale1, total1 * (1.0 / cells), cross1 * (1.0 / cells), sums_one


def pack_kernel(
    corr_ref, stat1_ref, par1_ref, sums1_ref, sums3_ref, proj_ref, out_ref, *, local_cells
):
    depth = proj_ref.shape[0]
    group = sums1_ref.shape[0]
    each = corr_ref.shape[0] // 3
    front, flat, tilt, sums_one = first_backward(
        stat1_ref, par1_ref, sums1_ref, local_cells, depth
    )
    blocks = []
    for k in range(3):
        at = k * each
        with_e = corr_ref[at : at + depth]
        with_n = corr_ref[at + depth : at + 2 * depth]
        with_one = corr_ref[at + 2 * depth : at + 2 * depth + 1]
        blocks.append(front * (with_e - flat * with_one - tilt * with_n))
    grad = jnp.concatenate(blocks, axis=0)
    tall = 3 * depth
    out_ref[0:tall] = grad[:, :128].astype(bf16)
    rest = grad[:, 128:]
    at = tall + tall // 2
    out_ref[tall:at] = jnp.concatenate([rest[: tall // 2], rest[tall // 2 :]], axis=1).astype(bf16)
    for k in range(0, proj_ref.shape[1], 128):
        out_ref[at : at + depth] = proj_ref[:, k : k + 128].astype(bf16)
        at += depth
    lines = list(sums_one)
    for kind in range(2):
        whole = summed_rows(sums3_ref, kind)
        lines += [whole[:, k : k + 128] for k in range(0, whole.shape[1], 128)]
    lines.append(jnp.zeros((8 - len(lines), 128), f32))
    small = jnp.concatenate(lines, axis=0) * (1.0 / group)
    high = small.astype(bf16).astype(f32)
    out_ref[at : at + 16] = jnp.concatenate([high, small - high], axis=0).astype(bf16)
    at += 16
    out_ref[at:] = jnp.zeros((out_ref.shape[0] - at, 128), bf16)


def back_kernel(
    e1_ref, n1_ref, row_ref, col_ref, corner_ref, stat1_ref, par1_ref, sums1_ref, w_ref,
    out_ref, shifted_ref,
):
    rows, depth, cols = e1_ref.shape
    front, flat, tilt, _ = first_backward(
        stat1_ref, par1_ref, sums1_ref, float(rows * cols), depth
    )
    front = spread_column(front, cols)
    flat = spread_column(flat, cols)
    tilt = spread_column(tilt, cols)

    def line_of(e1, n1):
        return front * (e1 - flat - n1 * tilt)

    lane = lax.broadcasted_iota(jnp.int32, (depth, cols), 1)
    _, half = place_flags()
    low = jnp.where(half == 1, 0, 1)
    high = jnp.where(half == 1, rows, rows + 1)
    side = col_ref[...] + corner_ref[...]
    side = jnp.where((lane >= low) & (lane <= high), line_of(side[:depth], side[depth:]), 0.0)
    three_shifts(
        lambda h: line_of(e1_ref[h], n1_ref[h]),
        line_of(row_ref[:depth], row_ref[depth:]), side, shifted_ref,
    )
    weights = w_ref[...]

    def body(j, carry):
        h = 2 * j
        both = conv_pair(weights, shifted_ref, h).astype(bf16)
        out_ref[h] = both[:, :cols]
        out_ref[h + 1] = both[:, cols:]
        return carry

    lax.fori_loop(0, rows // 2, body, 0, unroll=4)


def sum_kernel(parts_ref, out_ref):
    total = parts_ref[0].astype(f32)
    for d in range(1, parts_ref.shape[0]):
        total = total + parts_ref[d].astype(f32)
    total = total.astype(bf16)
    for d in range(parts_ref.shape[0]):
        out_ref[d] = total


def unpack_kernel(
    in_ref, conv_ref, proj_ref, gain1_ref, shift1_ref, gain3_ref, shift3_ref, *, factor
):
    depth, wide = proj_ref.shape
    tall = 3 * depth

    def take(start, stop):
        return in_ref[start:stop].astype(f32) * factor

    main = take(0, tall)
    at = tall + tall // 2
    rest = take(tall, at)
    rest = jnp.concatenate([rest[:, :depth], rest[:, depth:]], axis=0)
    for a in range(3):
        block = main[(2 - a) * depth : (3 - a) * depth]
        conv_ref[a, 0] = block[:, :depth]
        conv_ref[a, 1] = block[:, depth:]
        conv_ref[a, 2] = rest[(2 - a) * depth : (3 - a) * depth]
    for k in range(0, wide, 128):
        proj_ref[:, k : k + 128] = take(at, at + depth)
        at += depth
    both = take(at, at + 16)
    small = both[:8] + both[8:]
    shift1_ref[...] = small[0:1, :depth]
    gain1_ref[...] = small[1:2, :depth]
    steps = wide // 128
    for ref, start in ((shift3_ref, 2), (gain3_ref, 2 + steps)):
        for k in range(steps):
            ref[:, k * 128 : (k + 1) * 128] = small[start + k : start + k + 1]


def call(kernel, name, mib, outs, *args, scratch=()):
    return pl.pallas_call(
        kernel,
        out_shape=[jax.ShapeDtypeStruct(s, d) for s, d in outs],
        scratch_shapes=list(scratch),
        compiler_params=pltpu.CompilerParams(vmem_limit_bytes=mib * 1024 * 1024),
        name=name,
    )(*args)


def exchange(row, col, corner):
    return from_partner(row, 2), from_partner(col, 1), from_partner(corner, 3)


def swap(copies, axes):
    return lax.all_to_all(copies, axes, 0, 0)


def shards(
    images, out_grad, conv_weight, proj_weight, gain_one, shift_one, gain_three, shift_three
):
    depth, rows, cols = images.shape[2:]
    wide = out_grad.shape[2]
    group = lax.axis_size(group_axes)
    devices = lax.axis_size(all_axes)
    per_image = 1.0 / float(lax.axis_size("sp") * rows * cols)
    ahead = jnp.transpose(conv_weight, (2, 0, 1, 3)).reshape(depth, 9 * depth)
    behind = jnp.transpose(conv_weight[::-1, ::-1], (3, 0, 1, 2)).reshape(depth, 9 * depth)
    proj_t = proj_weight.T
    par_one = jnp.stack([gain_one, shift_one], axis=1)
    par_three = jnp.stack([gain_three, shift_three], axis=1)
    plane = (rows, depth, cols)
    piece = ((depth, cols), bf16)
    row_one = ((group, 8, max(depth, 128)), f32)
    row_three = ((group, 8, wide), f32)

    tall = pltpu.VMEM((depth * rows, cols), f32)
    keep = [pltpu.VMEM((5, wide, cols), f32)]
    lines, *edges = call(
        edge_kernel, "edges", EDGE, [(plane, bf16)] + [piece] * 3, images[0, 0], scratch=[tall]
    )
    (cotangent,) = call(
        lines_kernel, "lines", LINES, [((rows, wide, cols), bf16)], out_grad[0, 0], scratch=[tall]
    )
    shifted, conv_out, stat = call(
        conv_kernel, "conv", CONV,
        [((rows + 2, 3 * depth, cols), bf16), (plane, f32), row_one],
        lines, *exchange(*edges), ahead,
    )
    stat_one = swap(stat, group_axes)
    hidden, stat = call(
        hidden_kernel, "hidden", HIDDEN, [(plane, bf16), row_three],
        conv_out, stat_one, par_one, proj_weight,
        scratch=[pltpu.VMEM(plane, bf16)],
    )
    stat_three = swap(stat, group_axes)
    grad_out, sums = call(
        slope_kernel, "slope", SLOPE, [((rows, wide, cols), bf16), row_three],
        hidden, cotangent, stat_three, par_three, proj_t, scratch=keep,
    )
    sums_three = swap(sums, group_axes)
    pieces = ((2 * depth, cols), f32)
    grad_pre, normed, sums, proj, *edges = call(
        wide_kernel, "wide", WIDE,
        [(plane, f32), (plane, f32), row_one, ((depth, wide), f32)] + [pieces] * 3,
        hidden, grad_out, conv_out, stat_one, par_one, stat_three, par_three, sums_three,
        proj_t, proj_weight, scratch=keep,
    )
    sums_one = swap(sums, group_axes)
    edges = exchange(*edges)
    each = 2 * depth + 16
    (corr,) = call(
        corr_kernel, "corr", GRAD, [((3 * each, 3 * depth), f32)], grad_pre, normed, shifted,
        scratch=[pltpu.VMEM((rows + 4, each, cols), bf16)],
    )
    used = 9 * depth * depth // 128 + depth * wide // 128 + 16
    used += -used % (16 * 32)
    (part,) = call(
        partial(pack_kernel, local_cells=float(rows * cols)), "pack", PACK, [((used, 128), bf16)],
        corr, stat_one, par_one, sums_one, sums_three, proj,
    )
    (grad_field,) = call(
        back_kernel, "back", BACK, [(plane, bf16)],
        grad_pre, normed, *edges, stat_one, par_one, sums_one, behind,
        scratch=[pltpu.VMEM((rows + 2, 3 * depth, cols), bf16)],
    )
    part = jnp.pad(part, ((0, -used % (devices * 16)), (0, 0))).reshape(devices, -1, 128)
    parts = swap(part, all_axes)
    (mine,) = call(sum_kernel, "sum", 4, [(part.shape, bf16)], parts)
    full = swap(mine, all_axes).reshape(-1, 128)[:used]
    kernel_total, proj_total, gain1, shift1, gain3, shift3 = call(
        partial(unpack_kernel, factor=per_image), "unpack", 4,
        [((3, 3, depth, depth), f32), ((depth, wide), f32)]
        + [((1, depth), f32)] * 2 + [((1, wide), f32)] * 2,
        full,
    )
    return (
        jnp.transpose(grad_field, (1, 0, 2))[None, None],
        kernel_total,
        proj_total,
        gain1[0],
        shift1[0],
        gain3[0],
        shift3[0],
    )


def solution(mesh):
    in_specs = (
        P(("bn", "dp"), "sp", None, None, None),
        P(("bn", "dp"), "sp", None, None, None),
        P(),
        P(),
        P(),
        P(),
        P(),
        P(),
    )
    out_specs = (P(("bn", "dp"), "sp", None, None, None), P(), P(), P(), P(), P(), P())
    return jax.shard_map(shards, mesh=mesh, in_specs=in_specs, out_specs=out_specs, check_vma=False)
```

```python
from functools import partial

import jax
import jax.numpy as jnp
from jax import lax
from jax.experimental import pallas as pl
from jax.experimental.pallas import tpu as pltpu
from jax.sharding import PartitionSpec as P


norm_floor = 1e-05
bf16 = jnp.bfloat16
f32 = jnp.float32
EDGE, LINES, CONV, HIDDEN, SLOPE, WIDE, GRAD, PACK, BACK = 8, 16, 14, 12, 16, 24, 20, 4, 12
group_axes = ("sp", "bn")
all_axes = ("sp", "bn", "dp")


def from_partner(value, mask):
    return lax.ppermute(value, "sp", [(i, i ^ mask) for i in range(lax.axis_size("sp"))])


def nt_dot(left, right):
    return lax.dot_general(left, right, (((1,), (1,)), ((), ())), preferred_element_type=f32)


def nn_dot(left, right):
    return lax.dot_general(left, right, (((1,), (0,)), ((), ())), preferred_element_type=f32)


def lane_pair(ref, row):
    return jnp.concatenate([ref[row], ref[row + 1]], axis=1)


def fold_pair(value):
    half = value.shape[1] // 2
    return value[:, :half] + value[:, half:]


def row_of(partials):
    depth = partials.shape[0]
    if depth < 128:
        partials = jnp.concatenate([partials, jnp.zeros((128 - depth, 128), f32)], axis=0)
    pieces = [
        jnp.sum(jnp.transpose(partials[k : k + 128]), axis=0, keepdims=True)
        for k in range(0, partials.shape[0], 128)
    ]
    return pieces[0] if len(pieces) == 1 else jnp.concatenate(pieces, axis=1)


def columns_of(rows, depth):
    width = rows[0].shape[1]
    stacked = jnp.concatenate(rows + [jnp.zeros((128 - len(rows), width), f32)], axis=0)
    pieces = [jnp.transpose(stacked[:, k : k + 128]) for k in range(0, width, 128)]
    tall = pieces[0] if len(pieces) == 1 else jnp.concatenate(pieces, axis=0)
    return [tall[:depth, k : k + 1] for k in range(len(rows))]


def pack_rows(out_ref, rows):
    devices, height, width = out_ref.shape
    lines = [row[:, k : k + width] for row in rows for k in range(0, row.shape[1], width)]
    lines += [jnp.zeros((height - len(lines), width), f32)] if len(lines) < height else []
    block = jnp.concatenate(lines, axis=0)
    for d in range(devices):
        out_ref[d] = block


def row_at(gathered_ref, device, kind, depth):
    steps = max(depth // 128, 1)
    lines = [gathered_ref[device, k : k + 1, :] for k in range(kind * steps, (kind + 1) * steps)]
    return lines[0] if steps == 1 else jnp.concatenate(lines, axis=1)


def joined_moments(gathered_ref, local_cells, depth):
    devices = gathered_ref.shape[0]
    means = [row_at(gathered_ref, d, 0, depth) for d in range(devices)]
    average = sum(means[1:], means[0]) * (1.0 / devices)
    squares = None
    for d in range(devices):
        delta = means[d] - average
        term = row_at(gathered_ref, d, 1, depth) + local_cells * (delta * delta)
        squares = term if squares is None else squares + term
    return average, squares * (1.0 / (devices * local_cells))


def summed_rows(gathered_ref, kind, depth):
    total = row_at(gathered_ref, 0, kind, depth)
    for d in range(1, gathered_ref.shape[0]):
        total = total + row_at(gathered_ref, d, kind, depth)
    return total


def logistic(value):
    return 0.5 * jnp.tanh(0.5 * value) + 0.5


def place_flags():
    position = lax.axis_index("sp")
    return position % 2, position // 2


def edge_pieces(line_of, rows, shape, row_ref, col_ref, corner_ref, at=0):
    depth, cols = shape
    column, half = place_flags()
    lane = lax.broadcasted_iota(jnp.int32, (depth, cols), 1)
    edge = jnp.where(column == 0, cols - 1, 0)

    def body(h, found):
        moved = pltpu.roll(line_of(h), lax.rem(h + 1 - edge + cols, cols), 1)
        return jnp.where(lane == h + 1, moved, found)

    kind = row_ref.dtype
    block = pl.ds(at, depth)
    found = lax.fori_loop(0, rows, body, jnp.zeros((depth, cols), f32), unroll=4)
    col_ref[block] = found.astype(kind)
    border = line_of(jnp.where(half == 0, rows - 1, 0))
    row_ref[block] = border.astype(kind)
    target = jnp.where(half == 0, 0, rows + 1)
    moved = pltpu.roll(border, lax.rem(target - edge + cols, cols), 1)
    corner_ref[block] = jnp.where(lane == target, moved, 0.0).astype(kind)


def three_shifts(line_of, border, side, out_ref):
    rows = out_ref.shape[0] - 2
    depth, cols = border.shape
    column, half = place_flags()
    lane = lax.broadcasted_iota(jnp.int32, (depth, cols), 1)
    left = jnp.where(column == 1, side, 0.0)
    right = jnp.where(column == 0, side, 0.0)

    def place(r, line):
        before = pltpu.roll(line, 1, 1)
        after = pltpu.roll(line, cols - 1, 1)
        edge_left = pltpu.roll(left, (cols - r) % cols, 1)
        edge_right = pltpu.roll(right, (2 * cols - 1 - r) % cols, 1)
        before = jnp.where(lane == 0, edge_left, before)
        after = jnp.where(lane == cols - 1, edge_right, after)
        out_ref[r] = jnp.concatenate([before, line, after], axis=0).astype(bf16)

    place(0, jnp.where(half == 1, border, 0.0))
    place(rows + 1, jnp.where(half == 0, border, 0.0))

    def body(h, carry):
        place(h + 1, line_of(h))
        return carry

    lax.fori_loop(0, rows, body, 0, unroll=4)


def conv_pair(weights, shifted_ref, row):
    depth3 = shifted_ref.shape[1]
    cols = shifted_ref.shape[2]
    first = shifted_ref[pl.ds(row, 3)].reshape(3 * depth3, cols)
    second = shifted_ref[pl.ds(row + 1, 3)].reshape(3 * depth3, cols)
    return nn_dot(weights, jnp.concatenate([first, second], axis=1))


def to_lines(planes_ref, out_ref, tall_ref):
    depth, rows, _ = planes_ref.shape
    block = tall_ref.shape[0] // rows
    for start in range(0, depth, block):

        def spill(c, carry, start=start):
            at = pl.multiple_of(c * rows, 8)
            tall_ref[pl.ds(at, rows), :] = planes_ref[start + c].astype(f32)
            return carry

        lax.fori_loop(0, block, spill, 0, unroll=8)

        def collect(h, carry, start=start):
            line = tall_ref[pl.ds(h, block, stride=rows), :]
            out_ref[h, start : start + block] = line.astype(bf16)
            return carry

        lax.fori_loop(0, rows, collect, 0, unroll=4)


def edge_kernel(planes_ref, lines_ref, row_ref, col_ref, corner_ref, tall_ref):
    rows, depth, cols = lines_ref.shape
    to_lines(planes_ref, lines_ref, tall_ref)
    edge_pieces(
        lambda h: lines_ref[h].astype(f32), rows, (depth, cols), row_ref, col_ref, corner_ref
    )


def lines_kernel(planes_ref, lines_ref, tall_ref):
    to_lines(planes_ref, lines_ref, tall_ref)


def weights_kernel(conv_ref, proj_ref, ahead_ref, behind_ref, across_ref):
    depth, wide = proj_ref.shape
    blank = jnp.zeros((depth, 128 - depth), f32)

    def turned(block):
        block = jnp.concatenate([block, blank], axis=1) if depth < 128 else block
        tall = jnp.zeros((128 - depth, 128), f32)
        block = jnp.concatenate([block, tall], axis=0) if depth < 128 else block
        return jnp.transpose(block)[:depth, :depth]

    forth, back = [], []
    for a in range(3):
        for b in range(3):
            forth.append(conv_ref[a, b])
            back.append(turned(conv_ref[2 - a, 2 - b].astype(f32)).astype(bf16))
    ahead_ref[...] = jnp.concatenate(forth, axis=1)
    behind_ref[...] = jnp.concatenate(back, axis=1)
    for k in range(0, wide, 128):
        block = proj_ref[:, k : k + 128].astype(f32)
        block = jnp.concatenate([block, jnp.zeros((128 - depth, 128), f32)], axis=0)
        across_ref[k : k + 128] = jnp.transpose(block)[:, :depth].astype(bf16)


def conv_kernel(x_ref, row_ref, col_ref, corner_ref, w_ref, a_ref, stat_ref, shifted_ref):
    rows, depth, cols = x_ref.shape
    side = col_ref[...].astype(f32) + corner_ref[...].astype(f32)
    three_shifts(lambda h: x_ref[h].astype(f32), row_ref[...].astype(f32), side, shifted_ref)
    weights = w_ref[...]

    def body(j, total):
        h = 2 * j
        both = conv_pair(weights, shifted_ref, h)
        a_ref[h] = both[:, :cols]
        a_ref[h + 1] = both[:, cols:]
        return total + fold_pair(both)

    total = lax.fori_loop(0, rows // 2, body, jnp.zeros((depth, cols), f32), unroll=4)
    mean = jnp.sum(total, axis=1, keepdims=True) * (1.0 / (rows * cols))

    def spread(h, squares):
        centred = a_ref[h] - mean
        return squares + centred * centred

    squares = lax.fori_loop(0, rows, spread, jnp.zeros((depth, cols), f32), unroll=4)
    pack_rows(stat_ref, [row_of(total) * (1.0 / (rows * cols)), row_of(squares)])


def wide_row(ref):
    row = ref[...]
    short = -row.shape[1] % 128
    return jnp.concatenate([row, jnp.zeros((1, short), f32)], axis=1) if short else row


def norm_columns(gathered_ref, gain_ref, shift_ref, local_cells):
    depth = gain_ref.shape[1]
    average, variance = joined_moments(gathered_ref, local_cells, depth)
    scale = lax.rsqrt(variance + norm_floor)
    return columns_of([average, scale, wide_row(gain_ref), wide_row(shift_ref)], depth)


def spread_column(column, cols):
    return jnp.broadcast_to(column, (column.shape[0], cols))


def hidden_kernel(a_ref, stat_ref, gain_ref, shift_ref, w_ref, y_ref, out_ref, centred_ref):
    rows, depth, cols = a_ref.shape
    cells = float(rows * cols)
    mean, scale, gain, shift = norm_columns(stat_ref, gain_ref, shift_ref, cells)
    steep = spread_column(0.5 * gain * scale, cols)
    mean = spread_column(mean, cols)
    lift = spread_column(0.5 * shift, cols)
    middle = spread_column(shift * logistic(shift), cols).astype(bf16).astype(f32)

    def activate(h, total):
        half = (a_ref[h] - mean) * steep + lift
        hidden = (half + half * jnp.tanh(half)).astype(bf16)
        y_ref[h] = hidden
        centred = hidden.astype(f32) - middle
        centred_ref[h] = centred.astype(bf16)
        return total + centred

    total = lax.fori_loop(0, rows, activate, jnp.zeros((depth, cols), f32), unroll=4)
    gram = jnp.zeros((depth, depth), f32)
    step = 8
    for h in range(0, rows, step):
        wide_lines = jnp.concatenate([centred_ref[k] for k in range(h, min(h + step, rows))], axis=1)
        gram = gram + nt_dot(wide_lines, wide_lines)
    weights = w_ref[...].astype(f32)
    mean_c = jnp.sum(total, axis=1, keepdims=True) * (1.0 / cells)
    mean_r = row_of(total)[:, :depth] * (1.0 / cells)
    spread = gram - cells * (mean_c * mean_r)
    mixed = lax.dot_general(
        spread, weights, (((1,), (0,)), ((), ())),
        precision=lax.Precision.HIGHEST, preferred_element_type=f32,
    )
    squares = jnp.maximum(jnp.sum(mixed * weights, axis=0, keepdims=True), 0.0)
    means = jnp.sum(weights * (mean_c + middle[:, 0:1]), axis=0, keepdims=True)
    pack_rows(out_ref, [means, squares])


def slope_kernel(
    y_ref, g_ref, stat_ref, gain_ref, shift_ref, w_ref, e_ref, out_ref, keep_ref
):
    rows, _, cols = y_ref.shape
    wide = w_ref.shape[0]
    mean, scale, gain, shift = norm_columns(stat_ref, gain_ref, shift_ref, float(rows * cols))
    steep = 0.5 * gain * scale
    keep_ref[0] = spread_column(mean, cols)
    keep_ref[1] = spread_column(steep, cols)
    keep_ref[2] = spread_column(0.5 * shift, cols)
    keep_ref[3] = jnp.zeros((wide, cols), f32)
    keep_ref[4] = jnp.zeros((wide, cols), f32)
    block = 128

    def body(j, carry):
        h = 2 * j
        lines = lane_pair(y_ref, h)
        for start in range(0, wide, block):
            part = slice(start, start + block)
            both = nn_dot(w_ref[part], lines)
            m, s, b = keep_ref[0, part], keep_ref[1, part], keep_ref[2, part]
            total = cross = None
            for k in range(2):
                half = (both[:, k * cols : (k + 1) * cols] - m) * s + b
                t = jnp.tanh(half)
                slope = (1.0 + t) * (1.0 + half * (1.0 - t))
                grad = g_ref[h + k, part].astype(f32) * slope
                e_ref[h + k, part] = grad.astype(bf16)
                across = grad * half
                total = grad if total is None else total + grad
                cross = across if cross is None else cross + across
            keep_ref[3, part] += total
            keep_ref[4, part] += cross
        return carry

    lax.fori_loop(0, rows // 2, body, 0, unroll=2)
    total = row_of(keep_ref[3]) * 0.5
    cross = row_of(keep_ref[4])
    pack_rows(out_ref, [total, (cross - shift_ref[...] * total) / gain_ref[...]])


def wide_kernel(
    y_ref, e_ref, a_ref, stat1_ref, gain1_ref, shift1_ref, stat3_ref, gain3_ref, shift3_ref,
    sums_ref, w_ref, wt_ref,
    e1_ref, n1_ref, out_ref, proj_ref, row_ref, col_ref, corner_ref, keep_ref, db_ref,
):
    rows, depth, cols = y_ref.shape
    wide = w_ref.shape[0]
    local_cells = float(rows * cols)
    cells = local_cells * sums_ref.shape[0]
    mean3, scale3, gain3, _ = norm_columns(stat3_ref, gain3_ref, shift3_ref, local_cells)
    mean1, scale1, gain1, shift1 = norm_columns(stat1_ref, gain1_ref, shift1_ref, local_cells)
    total3, cross3 = columns_of(
        [summed_rows(sums_ref, 0, wide), summed_rows(sums_ref, 1, wide)], wide
    )
    front = gain3 * scale3
    tilt = front * scale3 * cross3 * (1.0 / cells)
    keep_ref[0] = spread_column(0.5 * front, cols)
    keep_ref[1] = spread_column(tilt, cols)
    keep_ref[2] = spread_column(front * total3 * (1.0 / cells) - tilt * mean3, cols)
    mean1 = spread_column(mean1, cols)
    scale1 = spread_column(scale1, cols)
    gain1 = spread_column(0.5 * gain1, cols)
    shift1 = spread_column(0.5 * shift1, cols)
    weights_t = wt_ref[...]
    block = 128

    def widen(j, carry):
        h = 2 * j
        hidden = lane_pair(y_ref, h)
        for start in range(0, wide, block):
            part = slice(start, start + block)
            both = nn_dot(w_ref[part], hidden)
            p, q, r = keep_ref[0, part], keep_ref[1, part], keep_ref[2, part]
            for k in range(2):
                grad = p * e_ref[h + k, part].astype(f32) - q * both[:, k * cols : (k + 1) * cols]
                db_ref[h + k, part] = (grad - r).astype(bf16)
        return carry

    lax.fori_loop(0, rows // 2, widen, 0, unroll=2)

    def narrow(j, carry):
        total, cross = carry
        h = 2 * j
        back = nn_dot(weights_t, lane_pair(db_ref, h))
        for k in range(2):
            normed = (a_ref[h + k] - mean1) * scale1
            half = gain1 * normed + shift1
            t = jnp.tanh(half)
            slope = (0.5 + 0.5 * t) * (1.0 + half * (1.0 - t))
            grad = back[:, k * cols : (k + 1) * cols] * slope
            e1_ref[h + k] = grad.astype(bf16)
            n1_ref[h + k] = normed.astype(bf16)
            total = total + grad
            cross = cross + grad * normed
        return total, cross

    zero = jnp.zeros((depth, cols), f32)
    total, cross = lax.fori_loop(0, rows // 2, narrow, (zero, zero), unroll=4)
    pack_rows(out_ref, [row_of(total), row_of(cross)])
    for ref, at in ((e1_ref, 0), (n1_ref, depth)):
        edge_pieces(
            lambda h, ref=ref: ref[h].astype(f32), rows, (depth, cols),
            row_ref, col_ref, corner_ref, at,
        )
    proj_ref[...] = jnp.zeros(proj_ref.shape, f32)
    step = 8
    for start in range(0, rows, step):
        lines = range(start, min(start + step, rows))
        left = jnp.concatenate([y_ref[h] for h in lines], axis=1)
        right = jnp.concatenate([db_ref[h] for h in lines], axis=1)
        proj_ref[...] += nt_dot(left, right)


def corr_kernel(
    e1_ref, n1_ref, x_ref, row_ref, col_ref, corner_ref, out_ref, padded_ref, shifted_ref
):
    rows, depth, cols = e1_ref.shape
    side = col_ref[...].astype(f32) + corner_ref[...].astype(f32)
    three_shifts(lambda h: x_ref[h].astype(f32), row_ref[...].astype(f32), side, shifted_ref)
    tall = padded_ref.shape[1]
    blank = jnp.zeros((2, tall, cols), bf16)
    padded_ref[pl.ds(0, 2)] = blank
    padded_ref[pl.ds(rows + 2, 2)] = blank
    ones = jnp.ones((tall - 2 * depth, cols), bf16)

    def fill(h, carry):
        padded_ref[h + 2] = jnp.concatenate(
            [e1_ref[h], n1_ref[h], ones], axis=0
        )
        return carry

    lax.fori_loop(0, rows, fill, 0, unroll=4)
    step = 6
    total = jnp.zeros(out_ref.shape, f32)
    out_ref[...] = total
    for start in range(0, rows + 2, step):
        lines = range(start, min(start + step, rows + 2))
        left = jnp.concatenate(
            [padded_ref[pl.ds(r, 3)].reshape(3 * tall, cols) for r in lines], axis=1
        )
        right = jnp.concatenate([shifted_ref[r] for r in lines], axis=1)
        out_ref[...] += nt_dot(left, right)


def first_backward(stat1_ref, gain1_ref, sums1_ref, local_cells):
    depth = gain1_ref.shape[1]
    cells = local_cells * sums1_ref.shape[0]
    _, scale1, gain1, _ = norm_columns(stat1_ref, gain1_ref, gain1_ref, local_cells)
    sums_one = [summed_rows(sums1_ref, 0, depth), summed_rows(sums1_ref, 1, depth)]
    total1, cross1 = columns_of(sums_one, depth)
    return gain1 * scale1, total1 * (1.0 / cells), cross1 * (1.0 / cells), sums_one


def pack_kernel(
    corr_ref, stat1_ref, gain1_ref, sums1_ref, sums3_ref, proj_ref, out_ref, *, local_cells
):
    depth = proj_ref.shape[0]
    group = sums1_ref.shape[0]
    each = corr_ref.shape[0] // 3
    front, flat, tilt, sums_one = first_backward(
        stat1_ref, gain1_ref, sums1_ref, local_cells
    )
    blocks = []
    for k in range(3):
        at = k * each
        with_e = corr_ref[at : at + depth]
        with_n = corr_ref[at + depth : at + 2 * depth]
        with_one = corr_ref[at + 2 * depth : at + 2 * depth + 1]
        blocks.append(front * (with_e - flat * with_one - tilt * with_n))
    grad = jnp.concatenate(blocks, axis=0)
    tall = 3 * depth
    out_ref[0:tall] = grad[:, :128].astype(bf16)
    rest = grad[:, 128:]
    at = tall + tall // 2
    out_ref[tall:at] = jnp.concatenate([rest[: tall // 2], rest[tall // 2 :]], axis=1).astype(bf16)
    for k in range(0, proj_ref.shape[1], 128):
        out_ref[at : at + depth] = proj_ref[:, k : k + 128].astype(bf16)
        at += depth
    lines = list(sums_one)
    for kind in range(2):
        whole = summed_rows(sums3_ref, kind, proj_ref.shape[1])
        lines += [whole[:, k : k + 128] for k in range(0, whole.shape[1], 128)]
    lines.append(jnp.zeros((8 - len(lines), 128), f32))
    small = jnp.concatenate(lines, axis=0) * (1.0 / group)
    high = small.astype(bf16).astype(f32)
    out_ref[at : at + 16] = jnp.concatenate([high, small - high], axis=0).astype(bf16)
    at += 16
    out_ref[at:] = jnp.zeros((out_ref.shape[0] - at, 128), bf16)


def back_kernel(
    e1_ref, n1_ref, row_ref, col_ref, corner_ref, stat1_ref, gain1_ref, sums1_ref, w_ref,
    out_ref, shifted_ref,
):
    rows, depth, cols = e1_ref.shape
    front, flat, tilt, _ = first_backward(
        stat1_ref, gain1_ref, sums1_ref, float(rows * cols)
    )
    front = spread_column(front, cols)
    flat = spread_column(flat, cols)
    tilt = spread_column(tilt, cols)

    def line_of(e1, n1):
        return front * (e1 - flat - n1 * tilt)

    lane = lax.broadcasted_iota(jnp.int32, (depth, cols), 1)
    _, half = place_flags()
    low = jnp.where(half == 1, 0, 1)
    high = jnp.where(half == 1, rows, rows + 1)
    side = col_ref[...].astype(f32) + corner_ref[...].astype(f32)
    side = jnp.where((lane >= low) & (lane <= high), line_of(side[:depth], side[depth:]), 0.0)
    three_shifts(
        lambda h: line_of(e1_ref[h].astype(f32), n1_ref[h].astype(f32)),
        line_of(row_ref[:depth].astype(f32), row_ref[depth:].astype(f32)), side, shifted_ref,
    )
    weights = w_ref[...]

    def body(j, carry):
        h = 2 * j
        both = conv_pair(weights, shifted_ref, h).astype(bf16)
        out_ref[h] = both[:, :cols]
        out_ref[h + 1] = both[:, cols:]
        return carry

    lax.fori_loop(0, rows // 2, body, 0, unroll=4)


def sum_kernel(parts_ref, out_ref):
    total = parts_ref[0].astype(f32)
    for d in range(1, parts_ref.shape[0]):
        total = total + parts_ref[d].astype(f32)
    total = total.astype(bf16)
    for d in range(parts_ref.shape[0]):
        out_ref[d] = total


def unpack_kernel(
    in_ref, conv_ref, proj_ref, gain1_ref, shift1_ref, gain3_ref, shift3_ref, *, factor
):
    depth, wide = proj_ref.shape
    tall = 3 * depth

    def take(start, stop):
        return in_ref[start:stop].astype(f32) * factor

    main = take(0, tall)
    at = tall + tall // 2
    rest = take(tall, at)
    rest = jnp.concatenate([rest[:, :depth], rest[:, depth:]], axis=0)
    for a in range(3):
        block = main[(2 - a) * depth : (3 - a) * depth]
        conv_ref[a, 0] = block[:, :depth]
        conv_ref[a, 1] = block[:, depth:]
        conv_ref[a, 2] = rest[(2 - a) * depth : (3 - a) * depth]
    for k in range(0, wide, 128):
        proj_ref[:, k : k + 128] = take(at, at + depth)
        at += depth
    both = take(at, at + 16)
    small = both[:8] + both[8:]
    shift1_ref[...] = small[0:1, :depth]
    gain1_ref[...] = small[1:2, :depth]
    steps = wide // 128
    for ref, start in ((shift3_ref, 2), (gain3_ref, 2 + steps)):
        for k in range(steps):
            ref[:, k * 128 : (k + 1) * 128] = small[start + k : start + k + 1]


def call(kernel, mib, outs, *args, scratch=()):
    return pl.pallas_call(
        kernel,
        out_shape=[jax.ShapeDtypeStruct(s, d) for s, d in outs],
        scratch_shapes=list(scratch),
        compiler_params=pltpu.CompilerParams(vmem_limit_bytes=mib * 1024 * 1024),
    )(*args)


def exchange(row, col, corner):
    return from_partner(row, 2), from_partner(col, 1), from_partner(corner, 3)


def swap(copies, axes):
    return lax.all_to_all(copies, axes, 0, 0)


def shards(
    images, out_grad, conv_weight, proj_weight, gain_one, shift_one, gain_three, shift_three
):
    depth, rows, cols = images.shape[2:]
    wide = out_grad.shape[2]
    group = lax.axis_size(group_axes)
    devices = lax.axis_size(all_axes)
    per_image = 1.0 / float(lax.axis_size("sp") * rows * cols)
    one = gain_one.reshape(1, -1), shift_one.reshape(1, -1)
    three = gain_three.reshape(1, -1), shift_three.reshape(1, -1)
    plane = (rows, depth, cols)
    piece = ((depth, cols), bf16)
    rows_out = ((group, 8, 128), f32)

    tall = pltpu.VMEM((depth * rows, cols), f32)
    keep = [pltpu.VMEM((5, wide, cols), f32)]
    lines, *edges = call(
        edge_kernel, EDGE, [(plane, bf16)] + [piece] * 3, images[0, 0], scratch=[tall]
    )
    (cotangent,) = call(
        lines_kernel, LINES, [((rows, wide, cols), bf16)], out_grad[0, 0], scratch=[tall]
    )
    ahead, behind, proj_t = call(
        weights_kernel, 4,
        [((depth, 9 * depth), bf16)] * 2 + [((wide, depth), bf16)], conv_weight, proj_weight,
    )
    edges = exchange(*edges)
    triple = pltpu.VMEM((rows + 2, 3 * depth, cols), bf16)
    conv_out, stat = call(
        conv_kernel, CONV, [(plane, f32), rows_out], lines, *edges, ahead, scratch=[triple]
    )
    stat_one = swap(stat, group_axes)
    hidden, stat = call(
        hidden_kernel, HIDDEN, [(plane, bf16), rows_out],
        conv_out, stat_one, *one, proj_weight,
        scratch=[pltpu.VMEM(plane, bf16)],
    )
    stat_three = swap(stat, group_axes)
    grad_out, sums = call(
        slope_kernel, SLOPE, [((rows, wide, cols), bf16), rows_out],
        hidden, cotangent, stat_three, *three, proj_t, scratch=keep,
    )
    sums_three = swap(sums, group_axes)
    pieces = ((2 * depth, cols), bf16)
    grad_pre, normed, sums, proj, *last = call(
        wide_kernel, WIDE,
        [(plane, bf16), (plane, bf16), rows_out, ((depth, wide), f32)] + [pieces] * 3,
        hidden, grad_out, conv_out, stat_one, *one, stat_three, *three, sums_three,
        proj_t, proj_weight, scratch=keep + [pltpu.VMEM((rows, wide, cols), bf16)],
    )
    sums_one = swap(sums, group_axes)
    last = exchange(*last)
    each = 2 * depth + 16
    (corr,) = call(
        corr_kernel, GRAD, [((3 * each, 3 * depth), f32)],
        grad_pre, normed, lines, *edges,
        scratch=[pltpu.VMEM((rows + 4, each, cols), bf16), triple],
    )
    used = 9 * depth * depth // 128 + depth * wide // 128 + 16
    used += -used % (16 * 32)
    (part,) = call(
        partial(pack_kernel, local_cells=float(rows * cols)), PACK, [((used, 128), bf16)],
        corr, stat_one, one[0], sums_one, sums_three, proj,
    )
    (grad_field,) = call(
        back_kernel, BACK, [(plane, bf16)],
        grad_pre, normed, *last, stat_one, one[0], sums_one, behind, scratch=[triple],
    )
    part = jnp.pad(part, ((0, -used % (devices * 16)), (0, 0))).reshape(devices, -1, 128)
    parts = swap(part, all_axes)
    (mine,) = call(sum_kernel, 4, [(part.shape, bf16)], parts)
    full = swap(mine, all_axes).reshape(-1, 128)[:used]
    kernel_total, proj_total, gain1, shift1, gain3, shift3 = call(
        partial(unpack_kernel, factor=per_image), 4,
        [((3, 3, depth, depth), f32), ((depth, wide), f32)]
        + [((1, depth), f32)] * 2 + [((1, wide), f32)] * 2,
        full,
    )
    return (
        jnp.transpose(grad_field, (1, 0, 2))[None, None],
        kernel_total,
        proj_total,
        gain1[0],
        shift1[0],
        gain3[0],
        shift3[0],
    )


def solution(mesh):
    in_specs = (
        P(("bn", "dp"), "sp", None, None, None),
        P(("bn", "dp"), "sp", None, None, None),
        P(),
        P(),
        P(),
        P(),
        P(),
        P(),
    )
    out_specs = (P(("bn", "dp"), "sp", None, None, None), P(), P(), P(), P(), P(), P())
    return jax.shard_map(shards, mesh=mesh, in_specs=in_specs, out_specs=out_specs, check_vma=False)
```

```python
from functools import partial

import jax
import jax.numpy as jnp
from jax import lax
from jax.experimental import pallas as pl
from jax.experimental.pallas import tpu as pltpu
from jax.sharding import PartitionSpec as P


norm_floor = 1e-05
bf16 = jnp.bfloat16
f32 = jnp.float32
EDGE, LINES, CONV, HIDDEN, SLOPE, WIDE, GRAD, BACK = 8, 16, 14, 12, 24, 16, 16, 12
group_axes = ("sp", "bn")
all_axes = ("sp", "bn", "dp")


def from_partner(value, mask):
    return lax.ppermute(value, "sp", [(i, i ^ mask) for i in range(lax.axis_size("sp"))])


def nt_dot(left, right):
    return lax.dot_general(left, right, (((1,), (1,)), ((), ())), preferred_element_type=f32)


def nn_dot(left, right):
    return lax.dot_general(left, right, (((1,), (0,)), ((), ())), preferred_element_type=f32)


def lane_pair(ref, row):
    return jnp.concatenate([ref[row], ref[row + 1]], axis=1)


def fold_pair(value):
    half = value.shape[1] // 2
    return value[:, :half] + value[:, half:]


def row_of(partials):
    depth = partials.shape[0]
    if depth < 128:
        partials = jnp.concatenate([partials, jnp.zeros((128 - depth, 128), f32)], axis=0)
    pieces = [
        jnp.sum(jnp.transpose(partials[k : k + 128]), axis=0, keepdims=True)
        for k in range(0, partials.shape[0], 128)
    ]
    return pieces[0] if len(pieces) == 1 else jnp.concatenate(pieces, axis=1)


def columns_of(rows, depth):
    width = rows[0].shape[1]
    stacked = jnp.concatenate(rows + [jnp.zeros((128 - len(rows), width), f32)], axis=0)
    pieces = [jnp.transpose(stacked[:, k : k + 128]) for k in range(0, width, 128)]
    tall = pieces[0] if len(pieces) == 1 else jnp.concatenate(pieces, axis=0)
    return [tall[:depth, k : k + 1] for k in range(len(rows))]


def pack_rows(out_ref, rows):
    devices, height, width = out_ref.shape
    lines = [row[:, k : k + width] for row in rows for k in range(0, row.shape[1], width)]
    lines += [jnp.zeros((height - len(lines), width), f32)] if len(lines) < height else []
    block = jnp.concatenate(lines, axis=0)
    for d in range(devices):
        out_ref[d] = block


def device_rows(gathered_ref):
    blocks = []
    for d in range(gathered_ref.shape[0]):
        if gathered_ref.dtype == f32:
            blocks.append(gathered_ref[d, 0:8])
        else:
            parts = gathered_ref[d, 0:32].astype(f32)
            blocks.append(parts[0:8] + parts[8:16] + parts[16:24])
    return blocks


def row_at(block, kind, depth):
    steps = max(depth // 128, 1)
    lines = [block[k : k + 1] for k in range(kind * steps, (kind + 1) * steps)]
    return lines[0] if steps == 1 else jnp.concatenate(lines, axis=1)


def joined_moments(gathered_ref, local_cells, depth):
    blocks = device_rows(gathered_ref)
    devices = len(blocks)
    means = [row_at(block, 0, depth) for block in blocks]
    average = sum(means[1:], means[0]) * (1.0 / devices)
    squares = None
    for block, mean in zip(blocks, means):
        delta = mean - average
        term = row_at(block, 1, depth) + local_cells * (delta * delta)
        squares = term if squares is None else squares + term
    return average, squares * (1.0 / (devices * local_cells))


def summed_block(gathered_ref):
    blocks = device_rows(gathered_ref)
    return sum(blocks[1:], blocks[0])


def place_flags():
    position = lax.axis_index("sp")
    return position % 2, position // 2


def edge_pieces(line_of, rows, shape, row_ref, col_ref, corner_ref, at=0):
    depth, cols = shape
    column, half = place_flags()
    lane = lax.broadcasted_iota(jnp.int32, (depth, cols), 1)
    edge = jnp.where(column == 0, cols - 1, 0)

    def body(h, found):
        moved = pltpu.roll(line_of(h), lax.rem(h + 1 - edge + cols, cols), 1)
        return jnp.where(lane == h + 1, moved, found)

    kind = row_ref.dtype
    block = pl.ds(at, depth)
    found = lax.fori_loop(0, rows, body, jnp.zeros((depth, cols), f32), unroll=4)
    col_ref[block] = found.astype(kind)
    border = line_of(jnp.where(half == 0, rows - 1, 0))
    row_ref[block] = border.astype(kind)
    target = jnp.where(half == 0, 0, rows + 1)
    moved = pltpu.roll(border, lax.rem(target - edge + cols, cols), 1)
    corner_ref[block] = jnp.where(lane == target, moved, 0.0).astype(kind)


def three_shifts(line_of, border, side, out_ref):
    rows = out_ref.shape[0] - 2
    depth, cols = border.shape
    column, half = place_flags()
    lane = lax.broadcasted_iota(jnp.int32, (depth, cols), 1)
    left = jnp.where(column == 1, side, 0.0)
    right = jnp.where(column == 0, side, 0.0)

    def place(r, line):
        before = pltpu.roll(line, 1, 1)
        after = pltpu.roll(line, cols - 1, 1)
        edge_left = pltpu.roll(left, (cols - r) % cols, 1)
        edge_right = pltpu.roll(right, (2 * cols - 1 - r) % cols, 1)
        before = jnp.where(lane == 0, edge_left, before)
        after = jnp.where(lane == cols - 1, edge_right, after)
        out_ref[r] = jnp.concatenate([before, line, after], axis=0).astype(bf16)

    place(0, jnp.where(half == 1, border, 0.0))
    place(rows + 1, jnp.where(half == 0, border, 0.0))

    def body(h, carry):
        place(h + 1, line_of(h))
        return carry

    lax.fori_loop(0, rows, body, 0, unroll=4)


def conv_pair(weights, shifted_ref, row):
    depth3 = shifted_ref.shape[1]
    cols = shifted_ref.shape[2]
    first = shifted_ref[pl.ds(row, 3)].reshape(3 * depth3, cols)
    second = shifted_ref[pl.ds(row + 1, 3)].reshape(3 * depth3, cols)
    return nn_dot(weights, jnp.concatenate([first, second], axis=1))


def to_lines(planes_ref, out_ref, tall_ref):
    depth, rows, _ = planes_ref.shape
    block = tall_ref.shape[0] // rows
    for start in range(0, depth, block):

        def spill(c, carry, start=start):
            at = pl.multiple_of(c * rows, 8)
            tall_ref[pl.ds(at, rows), :] = planes_ref[start + c].astype(f32)
            return carry

        lax.fori_loop(0, block, spill, 0, unroll=8)

        def collect(h, carry, start=start):
            line = tall_ref[pl.ds(h, block, stride=rows), :]
            out_ref[h, start : start + block] = line.astype(bf16)
            return carry

        lax.fori_loop(0, rows, collect, 0, unroll=4)


def edge_kernel(planes_ref, lines_ref, row_ref, col_ref, corner_ref, tall_ref):
    rows, depth, cols = lines_ref.shape
    to_lines(planes_ref, lines_ref, tall_ref)
    edge_pieces(
        lambda h: lines_ref[h].astype(f32), rows, (depth, cols), row_ref, col_ref, corner_ref
    )


def lines_kernel(planes_ref, lines_ref, tall_ref):
    to_lines(planes_ref, lines_ref, tall_ref)


def weights_kernel(conv_ref, proj_ref, ahead_ref, behind_ref, across_ref):
    depth, wide = proj_ref.shape
    blank = jnp.zeros((depth, 128 - depth), f32)

    def turned(block):
        block = jnp.concatenate([block, blank], axis=1) if depth < 128 else block
        tall = jnp.zeros((128 - depth, 128), f32)
        block = jnp.concatenate([block, tall], axis=0) if depth < 128 else block
        return jnp.transpose(block)[:depth, :depth]

    forth, back = [], []
    for a in range(3):
        for b in range(3):
            forth.append(conv_ref[a, b])
            back.append(turned(conv_ref[2 - a, 2 - b].astype(f32)).astype(bf16))
    ahead_ref[...] = jnp.concatenate(forth, axis=1)
    behind_ref[...] = jnp.concatenate(back, axis=1)
    for k in range(0, wide, 128):
        block = proj_ref[:, k : k + 128].astype(f32)
        block = jnp.concatenate([block, jnp.zeros((128 - depth, 128), f32)], axis=0)
        across_ref[k : k + 128] = jnp.transpose(block)[:, :depth].astype(bf16)


def conv_kernel(x_ref, row_ref, col_ref, corner_ref, w_ref, shifted_ref, a_ref, stat_ref):
    rows, depth, cols = x_ref.shape
    side = col_ref[...].astype(f32) + corner_ref[...].astype(f32)
    three_shifts(lambda h: x_ref[h].astype(f32), row_ref[...].astype(f32), side, shifted_ref)
    weights = w_ref[...]

    def body(j, total):
        h = 2 * j
        both = conv_pair(weights, shifted_ref, h)
        a_ref[h] = both[:, :cols]
        a_ref[h + 1] = both[:, cols:]
        return total + fold_pair(both)

    total = lax.fori_loop(0, rows // 2, body, jnp.zeros((depth, cols), f32), unroll=4)
    mean = jnp.sum(total, axis=1, keepdims=True) * (1.0 / (rows * cols))

    def spread(h, squares):
        centred = a_ref[h] - mean
        return squares + centred * centred

    squares = lax.fori_loop(0, rows, spread, jnp.zeros((depth, cols), f32), unroll=4)
    pack_rows(stat_ref, [row_of(total) * (1.0 / (rows * cols)), row_of(squares)])


def wide_row(ref):
    row = ref[...]
    short = -row.shape[1] % 128
    return jnp.concatenate([row, jnp.zeros((1, short), f32)], axis=1) if short else row


def norm_columns(gathered_ref, gain_ref, shift_ref, local_cells):
    depth = gain_ref.shape[1]
    average, variance = joined_moments(gathered_ref, local_cells, depth)
    scale = lax.rsqrt(variance + norm_floor)
    return columns_of([average, scale, wide_row(gain_ref), wide_row(shift_ref)], depth)


def spread_column(column, cols):
    return jnp.broadcast_to(column, (column.shape[0], cols))


def hidden_kernel(
    a_ref, stat_ref, gain_ref, shift_ref, w_ref,
    y_ref, turn_ref, out_ref, mixed_ref, mean_ref, centred_ref,
):
    rows, depth, cols = a_ref.shape
    cells = float(rows * cols)
    mean, scale, gain, shift = norm_columns(stat_ref, gain_ref, shift_ref, cells)
    gain = spread_column(0.5 * gain, cols)
    scale = spread_column(scale, cols)
    mean = spread_column(mean, cols)
    lift = spread_column(0.5 * shift, cols)
    rest = jnp.tanh(lift)
    middle = (lift + lift * rest).astype(bf16).astype(f32)
    level = (0.5 + 0.5 * rest) * (1.0 + lift * (1.0 - rest))

    def activate(h, carry):
        total, turned = carry
        normed = (a_ref[h] - mean) * scale
        half = normed * gain + lift
        t = jnp.tanh(half)
        hidden = (half + half * t).astype(bf16)
        slope = (0.5 + 0.5 * t) * (1.0 + half * (1.0 - t))
        turn = jnp.concatenate([slope - level, slope * normed], axis=0)
        turn_ref[h] = turn.astype(bf16)
        y_ref[h] = hidden
        centred = hidden.astype(f32) - middle
        centred_ref[h] = centred.astype(bf16)
        return total + centred, turned + turn

    zero = jnp.zeros((depth, cols), f32)
    both = jnp.zeros((2 * depth, cols), f32)
    total, turned = lax.fori_loop(0, rows, activate, (zero, both), unroll=4)
    gram = jnp.zeros((depth, 3 * depth), f32)
    step = 8
    for h in range(0, rows, step):
        lines = range(h, min(h + step, rows))
        left = jnp.concatenate([centred_ref[k] for k in lines], axis=1)
        right = jnp.concatenate([turn_ref[k] for k in lines], axis=1)
        gram = gram + nt_dot(left, jnp.concatenate([right, left], axis=0))
    across = gram[:, : 2 * depth]
    gram = gram[:, 2 * depth :]
    weights = w_ref[...].astype(f32)
    mean_c = jnp.sum(total, axis=1, keepdims=True) * (1.0 / cells)
    mean_r = row_of(total)[:, :depth] * (1.0 / cells)
    spread = gram - cells * (mean_c * mean_r)
    mixed = lax.dot_general(
        spread, weights, (((1,), (0,)), ((), ())),
        precision=lax.Precision.HIGHEST, preferred_element_type=f32,
    )
    mixed_ref[...] = mixed
    mean_ref[...] = mean_c + middle
    squares = jnp.maximum(jnp.sum(mixed * weights, axis=0, keepdims=True), 0.0)
    means = jnp.sum(weights * (mean_c + middle[:, 0:1]), axis=0, keepdims=True)
    width = out_ref.shape[2]
    lines = [row[:, k : k + width] for row in (means, squares) for k in range(0, row.shape[1], width)]
    lines.append(row_of(turned))
    block = jnp.concatenate(lines + [jnp.zeros((8 - len(lines), width), f32)], axis=0)
    high = block.astype(bf16).astype(f32)
    middle = (block - high).astype(bf16).astype(f32)
    low = block - high - middle
    block = jnp.concatenate([high, middle, low, jnp.zeros((8, width), f32), across], axis=0)
    block = block.astype(bf16)
    for d in range(out_ref.shape[0]):
        out_ref[d] = block


def slope_kernel(
    y_ref, g_ref, turn_ref, stat_ref, gain_ref, shift_ref, w_ref, wt_ref,
    f_ref, proj_ref, out_ref, keep_ref, e_ref,
):
    rows, depth, cols = y_ref.shape
    wide = w_ref.shape[0]
    mean, scale, gain, shift = norm_columns(stat_ref, gain_ref, shift_ref, float(rows * cols))
    steep = 0.5 * gain * scale
    keep_ref[0] = spread_column(mean, cols)
    keep_ref[1] = spread_column(steep, cols)
    keep_ref[2] = spread_column(0.5 * shift, cols)
    keep_ref[3] = jnp.zeros((wide, cols), f32)
    keep_ref[4] = jnp.zeros((wide, cols), f32)
    block = 128
    weights_t = wt_ref[...]

    def body(j, carry):
        h = 2 * j
        lines = lane_pair(y_ref, h)
        for start in range(0, wide, block):
            part = slice(start, start + block)
            both = nn_dot(w_ref[part], lines)
            m, s, b = keep_ref[0, part], keep_ref[1, part], keep_ref[2, part]
            total = cross = None
            for k in range(2):
                half = (both[:, k * cols : (k + 1) * cols] - m) * s + b
                t = jnp.tanh(half)
                slope = (1.0 + t) * (1.0 + half * (1.0 - t))
                grad = g_ref[h + k, part].astype(f32) * slope
                e_ref[h + k, part] = (grad * s).astype(bf16)
                across = grad * half
                total = grad if total is None else total + grad
                cross = across if cross is None else cross + across
            keep_ref[3, part] += total
            keep_ref[4, part] += cross
        return carry

    lax.fori_loop(0, rows // 2, body, 0, unroll=2)

    depth2 = 2 * depth

    def narrow(j, turned):
        h = 2 * j
        both = nn_dot(weights_t, lane_pair(e_ref, h))
        for k in range(2):
            line = both[:, k * cols : (k + 1) * cols]
            f_ref[h + k] = line
            turned = turned + jnp.concatenate([line, line], axis=0) * turn_ref[h + k].astype(f32)
        return turned

    turned = lax.fori_loop(0, rows // 2, narrow, jnp.zeros((depth2, cols), f32), unroll=4)
    proj_ref[...] = jnp.zeros(proj_ref.shape, f32)
    step = 8
    for start in range(0, rows, step):
        lines = range(start, min(start + step, rows))
        left = jnp.concatenate([y_ref[h] for h in lines], axis=1)
        right = jnp.concatenate([e_ref[h] for h in lines], axis=1)
        proj_ref[...] += nt_dot(left, right)
    total = row_of(keep_ref[3]) * 0.5
    cross = row_of(keep_ref[4])
    cross = (cross - shift_ref[...] * total) / gain_ref[...]
    pack_rows(out_ref, [total, cross, row_of(turned)])


def wide_kernel(
    y_ref, f_ref, a_ref, stat1_ref, gain1_ref, shift1_ref, stat3_ref, gain3_ref, sums_ref,
    wt_ref, mixed_ref, mean_ref, part_ref,
    da_ref, row_ref, col_ref, corner_ref, proj_ref, small_ref,
):
    rows, depth, cols = y_ref.shape
    wide = wt_ref.shape[1]
    local_cells = float(rows * cols)
    devices = sums_ref.shape[0]
    cells = local_cells * devices
    mean3, variance3 = joined_moments(stat3_ref, local_cells, wide)
    scale3 = lax.rsqrt(variance3 + norm_floor)
    front = gain3_ref[...] * scale3
    sums = summed_block(sums_ref)
    steps = wide // 128
    q = front * scale3 * row_at(sums, 1, wide) * (1.0 / cells)
    r = front * row_at(sums, 0, wide) * (1.0 / cells) - q * mean3
    weights = wt_ref[...].astype(f32)
    exact = lax.Precision.HIGHEST
    mixer = lax.dot_general(
        weights * q, weights, (((1,), (1,)), ((), ())),
        precision=exact, preferred_element_type=f32,
    )
    level_row = lax.dot_general(
        jnp.broadcast_to(r, (8, wide)), weights, (((1,), (1,)), ((), ())),
        precision=exact, preferred_element_type=f32,
    )[0:1]
    mean1, scale1, gain1, shift1 = norm_columns(stat1_ref, gain1_ref, shift1_ref, local_cells)
    lift = 0.5 * shift1
    middle = (lift + lift * jnp.tanh(lift)).astype(bf16).astype(f32)
    level_row = level_row + jnp.sum(mixer * middle, axis=0, keepdims=True)
    across = stat3_ref[0, 32 : 32 + depth].astype(f32)
    for d in range(1, devices):
        across = across + stat3_ref[d, 32 : 32 + depth].astype(f32)
    turned = summed_block(stat3_ref)[2 * steps : 2 * steps + 1]
    double = jnp.concatenate([mixer, mixer], axis=1)
    sums_one = sums[2 * steps : 2 * steps + 1] - jnp.sum(double * across, axis=0, keepdims=True)
    sums_one = sums_one - jnp.concatenate([level_row, level_row], axis=1) * turned
    blank = jnp.zeros((8 - 1 - 2 * steps, 128), f32)
    small_ref[...] = jnp.concatenate([sums_one, sums[: 2 * steps], blank], axis=0) * (1.0 / devices)
    (column,) = columns_of([sums_one], 2 * depth)
    back_front = spread_column(gain1 * scale1, cols)
    flat = spread_column(column[:depth] * (1.0 / cells), cols)
    tilt = spread_column(column[depth:] * (1.0 / cells), cols)
    mixer_high = mixer.astype(bf16)
    mixer = jnp.concatenate([mixer_high, (mixer - mixer_high.astype(f32)).astype(bf16)], axis=1)
    level = spread_column(jnp.sum(weights * r, axis=1, keepdims=True), cols)
    mean_y = mean_ref[:, 0:1]
    mean_b = jnp.sum(weights * mean_y, axis=0, keepdims=True)
    proj_ref[...] = part_ref[...] - q * mixed_ref[...] - (local_cells * mean_y) * (q * mean_b + r)
    mean1 = spread_column(mean1, cols)
    scale1 = spread_column(scale1, cols)
    gain1 = spread_column(0.5 * gain1, cols)
    shift1 = spread_column(lift, cols)

    def narrow(j, carry):
        h = 2 * j
        lines = lane_pair(y_ref, h)
        back = nn_dot(mixer, jnp.concatenate([lines, lines], axis=0))
        for k in range(2):
            normed = (a_ref[h + k] - mean1) * scale1
            half = gain1 * normed + shift1
            t = jnp.tanh(half)
            slope = (0.5 + 0.5 * t) * (1.0 + half * (1.0 - t))
            grad = (f_ref[h + k] - back[:, k * cols : (k + 1) * cols] - level) * slope
            da_ref[h + k] = (back_front * (grad - flat - normed * tilt)).astype(bf16)
        return carry

    lax.fori_loop(0, rows // 2, narrow, 0, unroll=4)
    edge_pieces(
        lambda h: da_ref[h].astype(f32), rows, (depth, cols), row_ref, col_ref, corner_ref
    )


def corr_kernel(da_ref, shifted_ref, proj_ref, small_ref, out_ref, padded_ref):
    rows, depth, cols = da_ref.shape
    blank = jnp.zeros((2, depth, cols), bf16)
    padded_ref[pl.ds(0, 2)] = blank
    padded_ref[pl.ds(rows + 2, 2)] = blank

    def fill(h, carry):
        padded_ref[h + 2] = da_ref[h]
        return carry

    lax.fori_loop(0, rows, fill, 0, unroll=8)
    tall = 3 * depth
    step = 6
    grad = jnp.zeros((tall, tall), f32)
    for start in range(0, rows + 2, step):
        lines = range(start, min(start + step, rows + 2))
        left = jnp.concatenate(
            [padded_ref[pl.ds(r, 3)].reshape(tall, cols) for r in lines], axis=1
        )
        right = jnp.concatenate([shifted_ref[r] for r in lines], axis=1)
        grad = grad + nt_dot(left, right)
    out_ref[0:tall] = grad[:, :128].astype(bf16)
    rest = grad[:, 128:]
    at = tall + tall // 2
    out_ref[tall:at] = jnp.concatenate([rest[: tall // 2], rest[tall // 2 :]], axis=1).astype(bf16)
    for k in range(0, proj_ref.shape[1], 128):
        out_ref[at : at + depth] = proj_ref[:, k : k + 128].astype(bf16)
        at += depth
    small = small_ref[...]
    high = small.astype(bf16).astype(f32)
    out_ref[at : at + 16] = jnp.concatenate([high, small - high], axis=0).astype(bf16)
    at += 16
    out_ref[at:] = jnp.zeros((out_ref.shape[0] - at, 128), bf16)


def back_kernel(d_ref, row_ref, col_ref, corner_ref, w_ref, out_ref, shifted_ref):
    rows, _, cols = d_ref.shape
    side = col_ref[...].astype(f32) + corner_ref[...].astype(f32)
    three_shifts(lambda h: d_ref[h].astype(f32), row_ref[...].astype(f32), side, shifted_ref)
    weights = w_ref[...]

    def body(j, carry):
        h = 2 * j
        both = conv_pair(weights, shifted_ref, h).astype(bf16)
        out_ref[h] = both[:, :cols]
        out_ref[h + 1] = both[:, cols:]
        return carry

    lax.fori_loop(0, rows // 2, body, 0, unroll=4)


def sum_kernel(parts_ref, out_ref):
    total = parts_ref[0].astype(f32)
    for d in range(1, parts_ref.shape[0]):
        total = total + parts_ref[d].astype(f32)
    total = total.astype(bf16)
    for d in range(parts_ref.shape[0]):
        out_ref[d] = total


def unpack_kernel(
    in_ref, conv_ref, proj_ref, gain1_ref, shift1_ref, gain3_ref, shift3_ref, *, factor
):
    depth, wide = proj_ref.shape
    tall = 3 * depth

    def take(start, stop):
        return in_ref[start:stop].astype(f32) * factor

    main = take(0, tall)
    at = tall + tall // 2
    rest = take(tall, at)
    rest = jnp.concatenate([rest[:, :depth], rest[:, depth:]], axis=0)
    for a in range(3):
        block = main[(2 - a) * depth : (3 - a) * depth]
        conv_ref[a, 0] = block[:, :depth]
        conv_ref[a, 1] = block[:, depth:]
        conv_ref[a, 2] = rest[(2 - a) * depth : (3 - a) * depth]
    for k in range(0, wide, 128):
        proj_ref[:, k : k + 128] = take(at, at + depth)
        at += depth
    both = take(at, at + 16)
    small = both[:8] + both[8:]
    shift1_ref[...] = small[0:1, :depth]
    gain1_ref[...] = small[0:1, depth : 2 * depth]
    steps = wide // 128
    for ref, start in ((shift3_ref, 1), (gain3_ref, 1 + steps)):
        for k in range(steps):
            ref[:, k * 128 : (k + 1) * 128] = small[start + k : start + k + 1]


def call(kernel, mib, outs, *args, scratch=()):
    return pl.pallas_call(
        kernel,
        out_shape=[jax.ShapeDtypeStruct(s, d) for s, d in outs],
        scratch_shapes=list(scratch),
        compiler_params=pltpu.CompilerParams(vmem_limit_bytes=mib * 1024 * 1024),
    )(*args)


def exchange(row, col, corner):
    return from_partner(row, 2), from_partner(col, 1), from_partner(corner, 3)


def swap(copies, axes):
    return lax.all_to_all(copies, axes, 0, 0)


def shards(
    images, out_grad, conv_weight, proj_weight, gain_one, shift_one, gain_three, shift_three
):
    depth, rows, cols = images.shape[2:]
    wide = out_grad.shape[2]
    group = lax.axis_size(group_axes)
    devices = lax.axis_size(all_axes)
    per_image = 1.0 / float(lax.axis_size("sp") * rows * cols)
    one = gain_one.reshape(1, -1), shift_one.reshape(1, -1)
    three = gain_three.reshape(1, -1), shift_three.reshape(1, -1)
    plane = (rows, depth, cols)
    piece = ((depth, cols), bf16)
    rows_out = ((group, 8, 128), f32)

    tall = pltpu.VMEM((depth * rows, cols), f32)
    keep = [pltpu.VMEM((5, wide, cols), f32)]
    lines, *edges = call(
        edge_kernel, EDGE, [(plane, bf16)] + [piece] * 3, images[0, 0], scratch=[tall]
    )
    (cotangent,) = call(
        lines_kernel, LINES, [((rows, wide, cols), bf16)], out_grad[0, 0], scratch=[tall]
    )
    ahead, behind, proj_t = call(
        weights_kernel, 4,
        [((depth, 9 * depth), bf16)] * 2 + [((wide, depth), bf16)], conv_weight, proj_weight,
    )
    edges = exchange(*edges)
    triple = pltpu.VMEM((rows + 2, 3 * depth, cols), bf16)
    shifted, conv_out, stat = call(
        conv_kernel, CONV,
        [((rows + 2, 3 * depth, cols), bf16), (plane, f32), rows_out], lines, *edges, ahead,
    )
    stat_one = swap(stat, group_axes)
    hidden, turn, stat, mixed, mean_y = call(
        hidden_kernel, HIDDEN,
        [(plane, bf16), ((rows, 2 * depth, cols), bf16), ((group, 32 + depth, 128), bf16)]
        + [((depth, wide), f32), ((depth, cols), f32)],
        conv_out, stat_one, *one, proj_weight,
        scratch=[pltpu.VMEM(plane, bf16)],
    )
    stat_three = swap(stat, group_axes)
    narrowed, part, sums = call(
        slope_kernel, SLOPE, [(plane, f32), ((depth, wide), f32), rows_out],
        hidden, cotangent, turn, stat_three, *three, proj_t, proj_weight,
        scratch=keep + [pltpu.VMEM((rows, wide, cols), bf16)],
    )
    sums_three = swap(sums, group_axes)
    grad_conv, *last, proj, small = call(
        wide_kernel, WIDE,
        [(plane, bf16)] + [piece] * 3 + [((depth, wide), f32), ((8, 128), f32)],
        hidden, narrowed, conv_out, stat_one, *one, stat_three, three[0], sums_three,
        proj_weight, mixed, mean_y, part,
    )
    last = exchange(*last)
    used = 9 * depth * depth // 128 + depth * wide // 128 + 16
    used += -used % (16 * 32)
    (part,) = call(
        corr_kernel, GRAD, [((used, 128), bf16)], grad_conv, shifted, proj, small,
        scratch=[pltpu.VMEM((rows + 4, depth, cols), bf16)],
    )
    (grad_field,) = call(
        back_kernel, BACK, [(plane, bf16)], grad_conv, *last, behind, scratch=[triple]
    )
    part = jnp.pad(part, ((0, -used % (devices * 16)), (0, 0))).reshape(devices, -1, 128)
    parts = swap(part, all_axes)
    (mine,) = call(sum_kernel, 4, [(part.shape, bf16)], parts)
    full = swap(mine, all_axes).reshape(-1, 128)[:used]
    kernel_total, proj_total, gain1, shift1, gain3, shift3 = call(
        partial(unpack_kernel, factor=per_image), 4,
        [((3, 3, depth, depth), f32), ((depth, wide), f32)]
        + [((1, depth), f32)] * 2 + [((1, wide), f32)] * 2,
        full,
    )
    return (
        jnp.transpose(grad_field, (1, 0, 2))[None, None],
        kernel_total,
        proj_total,
        gain1[0],
        shift1[0],
        gain3[0],
        shift3[0],
    )


def solution(mesh):
    in_specs = (
        P(("bn", "dp"), "sp", None, None, None),
        P(("bn", "dp"), "sp", None, None, None),
        P(),
        P(),
        P(),
        P(),
        P(),
        P(),
    )
    out_specs = (P(("bn", "dp"), "sp", None, None, None), P(), P(), P(), P(), P(), P())
    return jax.shard_map(shards, mesh=mesh, in_specs=in_specs, out_specs=out_specs, check_vma=False)
```

```python
from functools import partial

import jax
import jax.numpy as jnp
from jax import lax
from jax.experimental import pallas as pl
from jax.experimental.pallas import tpu as pltpu
from jax.sharding import PartitionSpec as P


norm_floor = 1e-05
bf16 = jnp.bfloat16
f32 = jnp.float32
EDGE, LINES, CONV, HIDDEN, SLOPE, WIDE, GRAD, BACK = 8, 16, 14, 12, 24, 16, 16, 12
group_axes = ("sp", "bn")
all_axes = ("sp", "bn", "dp")


def from_partner(value, mask):
    return lax.ppermute(value, "sp", [(i, i ^ mask) for i in range(lax.axis_size("sp"))])


def nt_dot(left, right):
    return lax.dot_general(left, right, (((1,), (1,)), ((), ())), preferred_element_type=f32)


def nn_dot(left, right):
    return lax.dot_general(left, right, (((1,), (0,)), ((), ())), preferred_element_type=f32)


def lane_pair(ref, row):
    return jnp.concatenate([ref[row], ref[row + 1]], axis=1)


def row_of(partials):
    depth = partials.shape[0]
    if depth < 128:
        partials = jnp.concatenate([partials, jnp.zeros((128 - depth, 128), f32)], axis=0)
    pieces = [
        jnp.sum(jnp.transpose(partials[k : k + 128]), axis=0, keepdims=True)
        for k in range(0, partials.shape[0], 128)
    ]
    return pieces[0] if len(pieces) == 1 else jnp.concatenate(pieces, axis=1)


def columns_of(rows, depth):
    width = rows[0].shape[1]
    stacked = jnp.concatenate(rows + [jnp.zeros((128 - len(rows), width), f32)], axis=0)
    pieces = [jnp.transpose(stacked[:, k : k + 128]) for k in range(0, width, 128)]
    tall = pieces[0] if len(pieces) == 1 else jnp.concatenate(pieces, axis=0)
    return [tall[:depth, k : k + 1] for k in range(len(rows))]


def pack_rows(out_ref, rows):
    devices, height, width = out_ref.shape
    lines = [row[:, k : k + width] for row in rows for k in range(0, row.shape[1], width)]
    lines += [jnp.zeros((height - len(lines), width), f32)] if len(lines) < height else []
    block = jnp.concatenate(lines, axis=0)
    for d in range(devices):
        out_ref[d] = block


def device_rows(gathered_ref):
    blocks = []
    for d in range(gathered_ref.shape[0]):
        if gathered_ref.dtype == f32:
            blocks.append(gathered_ref[d, 0:8])
        else:
            parts = gathered_ref[d, 0:32].astype(f32)
            blocks.append(parts[0:8] + parts[8:16] + parts[16:24])
    return blocks


def row_at(block, kind, depth):
    steps = max(depth // 128, 1)
    lines = [block[k : k + 1] for k in range(kind * steps, (kind + 1) * steps)]
    return lines[0] if steps == 1 else jnp.concatenate(lines, axis=1)


def joined_moments(gathered_ref, local_cells, depth):
    blocks = device_rows(gathered_ref)
    devices = len(blocks)
    means = [row_at(block, 0, depth) for block in blocks]
    average = sum(means[1:], means[0]) * (1.0 / devices)
    squares = None
    for block, mean in zip(blocks, means):
        delta = mean - average
        term = row_at(block, 1, depth) + local_cells * (delta * delta)
        squares = term if squares is None else squares + term
    return average, squares * (1.0 / (devices * local_cells))


def summed_block(gathered_ref):
    blocks = device_rows(gathered_ref)
    return sum(blocks[1:], blocks[0])


def place_flags():
    position = lax.axis_index("sp")
    return position % 2, position // 2


def edge_pieces(line_of, rows, shape, row_ref, col_ref, corner_ref, at=0):
    depth, cols = shape
    column, half = place_flags()
    lane = lax.broadcasted_iota(jnp.int32, (depth, cols), 1)
    edge = jnp.where(column == 0, cols - 1, 0)

    def body(h, found):
        moved = pltpu.roll(line_of(h), lax.rem(h + 1 - edge + cols, cols), 1)
        return jnp.where(lane == h + 1, moved, found)

    kind = row_ref.dtype
    block = pl.ds(at, depth)
    found = lax.fori_loop(0, rows, body, jnp.zeros((depth, cols), f32), unroll=rows)
    col_ref[block] = found.astype(kind)
    border = line_of(jnp.where(half == 0, rows - 1, 0))
    row_ref[block] = border.astype(kind)
    target = jnp.where(half == 0, 0, rows + 1)
    moved = pltpu.roll(border, lax.rem(target - edge + cols, cols), 1)
    corner_ref[block] = jnp.where(lane == target, moved, 0.0).astype(kind)


def three_shifts(line_of, border, side, out_ref):
    rows = out_ref.shape[0] - 2
    depth, cols = border.shape
    column, half = place_flags()
    lane = lax.broadcasted_iota(jnp.int32, (depth, cols), 1)
    start = jnp.where(column == 1, cols, 2 * cols - 1)

    def place(r, line):
        before = pltpu.roll(line, 1, 1)
        after = pltpu.roll(line, cols - 1, 1)
        edge = pltpu.roll(side, lax.rem(start - r, cols), 1)
        before = jnp.where(lane == 0, jnp.where(column == 1, edge, 0.0), before)
        after = jnp.where(lane == cols - 1, jnp.where(column == 0, edge, 0.0), after)
        out_ref[r] = jnp.concatenate([before, line, after], axis=0).astype(bf16)

    place(0, jnp.where(half == 1, border, 0.0))
    place(rows + 1, jnp.where(half == 0, border, 0.0))

    def body(h, carry):
        place(h + 1, line_of(h))
        return carry

    lax.fori_loop(0, rows, body, 0, unroll=rows)


def conv_lines(weights, shifted_ref, row):
    depth3 = shifted_ref.shape[1]
    cols = shifted_ref.shape[2]
    depth = depth3 // 3
    first = shifted_ref[pl.ds(row, 4)].reshape(4 * depth3, cols)
    second = shifted_ref[pl.ds(row + 2, 4)].reshape(4 * depth3, cols)
    found = nn_dot(weights, jnp.concatenate([first, second], axis=1))
    return [
        found[u * depth : (u + 1) * depth, k * cols : (k + 1) * cols]
        for k in range(2)
        for u in range(2)
    ]


def to_lines(planes_ref, out_ref, tall_ref):
    depth, rows, _ = planes_ref.shape
    block = tall_ref.shape[0] // rows
    for start in range(0, depth, block):

        def spill(c, carry, start=start):
            at = pl.multiple_of(c * rows, 8)
            tall_ref[pl.ds(at, rows), :] = planes_ref[start + c].astype(f32)
            return carry

        lax.fori_loop(0, block, spill, 0, unroll=8)

        def collect(h, carry, start=start):
            line = tall_ref[pl.ds(h, block, stride=rows), :]
            out_ref[h, start : start + block] = line.astype(bf16)
            return carry

        lax.fori_loop(0, rows, collect, 0, unroll=rows)


def edge_kernel(planes_ref, lines_ref, row_ref, col_ref, corner_ref, tall_ref):
    rows, depth, cols = lines_ref.shape
    to_lines(planes_ref, lines_ref, tall_ref)
    edge_pieces(
        lambda h: lines_ref[h].astype(f32), rows, (depth, cols), row_ref, col_ref, corner_ref
    )


def lines_kernel(planes_ref, lines_ref, tall_ref):
    to_lines(planes_ref, lines_ref, tall_ref)


def weights_kernel(conv_ref, proj_ref, ahead_ref, behind_ref, across_ref):
    depth, wide = proj_ref.shape
    blank = jnp.zeros((depth, 128 - depth), f32)

    def turned(block):
        block = jnp.concatenate([block, blank], axis=1) if depth < 128 else block
        tall = jnp.zeros((128 - depth, 128), f32)
        block = jnp.concatenate([block, tall], axis=0) if depth < 128 else block
        return jnp.transpose(block)[:depth, :depth]

    forth, back = [], []
    for a in range(3):
        for b in range(3):
            forth.append(conv_ref[a, b])
            back.append(turned(conv_ref[2 - a, 2 - b].astype(f32)).astype(bf16))
    gap = [jnp.zeros((depth, depth), bf16)] * 3
    for ref, blocks in ((ahead_ref, forth), (behind_ref, back)):
        ref[:depth] = jnp.concatenate(blocks + gap, axis=1)
        ref[depth:] = jnp.concatenate(gap + blocks, axis=1)
    for k in range(0, wide, 128):
        block = proj_ref[:, k : k + 128].astype(f32)
        block = jnp.concatenate([block, jnp.zeros((128 - depth, 128), f32)], axis=0)
        across_ref[k : k + 128] = jnp.transpose(block)[:, :depth].astype(bf16)


def conv_kernel(x_ref, row_ref, col_ref, corner_ref, w_ref, shifted_ref, a_ref, stat_ref):
    rows, depth, cols = x_ref.shape
    side = col_ref[...].astype(f32) + corner_ref[...].astype(f32)
    three_shifts(lambda h: x_ref[h].astype(f32), row_ref[...].astype(f32), side, shifted_ref)
    weights = w_ref[...]

    def body(j, total):
        h = 4 * j
        for k, line in enumerate(conv_lines(weights, shifted_ref, h)):
            a_ref[h + k] = line
            total = total + line
        return total

    total = lax.fori_loop(0, rows // 4, body, jnp.zeros((depth, cols), f32), unroll=rows // 4)
    mean = jnp.sum(total, axis=1, keepdims=True) * (1.0 / (rows * cols))

    def spread(h, squares):
        centred = a_ref[h] - mean
        return squares + centred * centred

    squares = lax.fori_loop(0, rows, spread, jnp.zeros((depth, cols), f32), unroll=rows)
    pack_rows(stat_ref, [row_of(total) * (1.0 / (rows * cols)), row_of(squares)])


def wide_row(ref):
    row = ref[...]
    short = -row.shape[1] % 128
    return jnp.concatenate([row, jnp.zeros((1, short), f32)], axis=1) if short else row


def norm_columns(gathered_ref, gain_ref, shift_ref, local_cells):
    depth = gain_ref.shape[1]
    average, variance = joined_moments(gathered_ref, local_cells, depth)
    scale = lax.rsqrt(variance + norm_floor)
    return columns_of([average, scale, wide_row(gain_ref), wide_row(shift_ref)], depth)


def spread_column(column, cols):
    return jnp.broadcast_to(column, (column.shape[0], cols))


def hidden_kernel(
    a_ref, stat_ref, gain_ref, shift_ref, w_ref,
    y_ref, turn_ref, out_ref, mixed_ref, mean_ref, centred_ref,
):
    rows, depth, cols = a_ref.shape
    cells = float(rows * cols)
    mean, scale, gain, shift = norm_columns(stat_ref, gain_ref, shift_ref, cells)
    gain = spread_column(0.5 * gain, cols)
    scale = spread_column(scale, cols)
    mean = spread_column(mean, cols)
    lift = spread_column(0.5 * shift, cols)
    rest = jnp.tanh(lift)
    middle = (lift + lift * rest).astype(bf16).astype(f32)
    level = (0.5 + 0.5 * rest) * (1.0 + lift * (1.0 - rest))

    def activate(h, carry):
        total, turned = carry
        normed = (a_ref[h] - mean) * scale
        half = normed * gain + lift
        t = jnp.tanh(half)
        hidden = (half + half * t).astype(bf16)
        slope = (0.5 + 0.5 * t) * (1.0 + half * (1.0 - t))
        turn = jnp.concatenate([slope - level, slope * normed], axis=0)
        turn_ref[h] = turn.astype(bf16)
        y_ref[h] = hidden
        centred = hidden.astype(f32) - middle
        centred_ref[h] = centred.astype(bf16)
        return total + centred, turned + turn

    zero = jnp.zeros((depth, cols), f32)
    both = jnp.zeros((2 * depth, cols), f32)
    total, turned = lax.fori_loop(0, rows, activate, (zero, both), unroll=rows)
    gram = jnp.zeros((depth, 3 * depth), f32)
    step = 8
    for h in range(0, rows, step):
        lines = range(h, min(h + step, rows))
        left = jnp.concatenate([centred_ref[k] for k in lines], axis=1)
        right = jnp.concatenate([turn_ref[k] for k in lines], axis=1)
        gram = gram + nt_dot(left, jnp.concatenate([right, left], axis=0))
    across = gram[:, : 2 * depth]
    gram = gram[:, 2 * depth :]
    weights = w_ref[...].astype(f32)
    mean_c = jnp.sum(total, axis=1, keepdims=True) * (1.0 / cells)
    mean_r = row_of(total)[:, :depth] * (1.0 / cells)
    spread = gram - cells * (mean_c * mean_r)
    mixed = lax.dot_general(
        spread, weights, (((1,), (0,)), ((), ())),
        precision=lax.Precision.HIGHEST, preferred_element_type=f32,
    )
    mixed_ref[...] = mixed
    mean_ref[...] = mean_c + middle
    squares = jnp.maximum(jnp.sum(mixed * weights, axis=0, keepdims=True), 0.0)
    means = jnp.sum(weights * (mean_c + middle[:, 0:1]), axis=0, keepdims=True)
    width = out_ref.shape[2]
    lines = [row[:, k : k + width] for row in (means, squares) for k in range(0, row.shape[1], width)]
    lines.append(row_of(turned))
    block = jnp.concatenate(lines + [jnp.zeros((8 - len(lines), width), f32)], axis=0)
    high = block.astype(bf16).astype(f32)
    middle = (block - high).astype(bf16).astype(f32)
    low = block - high - middle
    block = jnp.concatenate([high, middle, low, jnp.zeros((8, width), f32), across], axis=0)
    block = block.astype(bf16)
    for d in range(out_ref.shape[0]):
        out_ref[d] = block


def slope_kernel(
    y_ref, g_ref, turn_ref, stat_ref, gain_ref, shift_ref, w_ref, wt_ref,
    f_ref, proj_ref, out_ref, keep_ref, e_ref,
):
    rows, depth, cols = y_ref.shape
    wide = w_ref.shape[0]
    mean, scale, gain, shift = norm_columns(stat_ref, gain_ref, shift_ref, float(rows * cols))
    steep = 0.5 * gain * scale
    keep_ref[0] = spread_column(steep, cols)
    keep_ref[1] = spread_column(0.5 * shift - mean * steep, cols)
    keep_ref[2] = jnp.zeros((wide, cols), f32)
    keep_ref[3] = jnp.zeros((wide, cols), f32)
    proj_ref[...] = jnp.zeros(proj_ref.shape, f32)
    block = 64
    weights_t = wt_ref[...]

    def expand(j):
        h = 2 * j
        lines = lane_pair(y_ref, h)
        for start in range(0, wide, block):
            part = slice(start, start + block)
            both = nn_dot(w_ref[part], lines)
            s, b = keep_ref[0, part], keep_ref[1, part]
            total = cross = None
            for k in range(2):
                half = both[:, k * cols : (k + 1) * cols] * s + b
                t = jnp.tanh(half)
                slope = (1.0 + t) * (1.0 + half * (1.0 - t))
                grad = g_ref[h + k, part].astype(f32) * slope
                e_ref[h + k, part] = (grad * s).astype(bf16)
                across = grad * half
                total = grad if total is None else total + grad
                cross = across if cross is None else cross + across
            keep_ref[2, part] += total
            keep_ref[3, part] += cross

    def narrow(j, turned):
        h = 2 * j
        scaled = lane_pair(e_ref, h)
        both = nn_dot(weights_t, scaled)
        proj_ref[...] += nt_dot(lane_pair(y_ref, h), scaled)
        for k in range(2):
            line = both[:, k * cols : (k + 1) * cols]
            f_ref[h + k] = line
            turned = turned + jnp.concatenate([line, line], axis=0) * turn_ref[h + k].astype(f32)
        return turned

    def body(j, turned):
        expand(j)
        turned = narrow(j - 1, turned)
        return turned

    expand(0)
    turned = jnp.zeros((2 * depth, cols), f32)
    turned = lax.fori_loop(1, rows // 2, body, turned, unroll=rows // 2 - 1)
    turned = narrow(rows // 2 - 1, turned)
    total = row_of(keep_ref[2]) * 0.5
    cross = row_of(keep_ref[3])
    cross = (cross - shift_ref[...] * total) / gain_ref[...]
    pack_rows(out_ref, [total, cross, row_of(turned)])


def wide_kernel(
    y_ref, f_ref, a_ref, stat1_ref, gain1_ref, shift1_ref, stat3_ref, gain3_ref, sums_ref,
    wt_ref, mixed_ref, mean_ref, part_ref,
    da_ref, row_ref, col_ref, corner_ref, proj_ref, small_ref,
):
    rows, depth, cols = y_ref.shape
    wide = wt_ref.shape[1]
    local_cells = float(rows * cols)
    devices = sums_ref.shape[0]
    cells = local_cells * devices
    mean3, variance3 = joined_moments(stat3_ref, local_cells, wide)
    scale3 = lax.rsqrt(variance3 + norm_floor)
    front = gain3_ref[...] * scale3
    sums = summed_block(sums_ref)
    steps = wide // 128
    q = front * scale3 * row_at(sums, 1, wide) * (1.0 / cells)
    r = front * row_at(sums, 0, wide) * (1.0 / cells) - q * mean3
    weights = wt_ref[...].astype(f32)
    exact = lax.Precision.HIGHEST
    mixer = lax.dot_general(
        weights * q, weights, (((1,), (1,)), ((), ())),
        precision=exact, preferred_element_type=f32,
    )
    level_row = lax.dot_general(
        jnp.broadcast_to(r, (8, wide)), weights, (((1,), (1,)), ((), ())),
        precision=exact, preferred_element_type=f32,
    )[0:1]
    mean1, scale1, gain1, shift1 = norm_columns(stat1_ref, gain1_ref, shift1_ref, local_cells)
    lift = 0.5 * shift1
    middle = (lift + lift * jnp.tanh(lift)).astype(bf16).astype(f32)
    level_row = level_row + jnp.sum(mixer * middle, axis=0, keepdims=True)
    across = stat3_ref[0, 32 : 32 + depth].astype(f32)
    for d in range(1, devices):
        across = across + stat3_ref[d, 32 : 32 + depth].astype(f32)
    turned = summed_block(stat3_ref)[2 * steps : 2 * steps + 1]
    double = jnp.concatenate([mixer, mixer], axis=1)
    sums_one = sums[2 * steps : 2 * steps + 1] - jnp.sum(double * across, axis=0, keepdims=True)
    sums_one = sums_one - jnp.concatenate([level_row, level_row], axis=1) * turned
    blank = jnp.zeros((8 - 1 - 2 * steps, 128), f32)
    small_ref[...] = jnp.concatenate([sums_one, sums[: 2 * steps], blank], axis=0) * (1.0 / devices)
    (column,) = columns_of([sums_one], 2 * depth)
    back_front = spread_column(gain1 * scale1, cols)
    flat = spread_column(column[:depth] * (1.0 / cells), cols)
    tilt = spread_column(column[depth:] * (1.0 / cells), cols)
    mixer_high = mixer.astype(bf16)
    mixer = jnp.concatenate([mixer_high, (mixer - mixer_high.astype(f32)).astype(bf16)], axis=1)
    level = spread_column(jnp.sum(weights * r, axis=1, keepdims=True), cols)
    mean_y = mean_ref[:, 0:1]
    mean_b = jnp.sum(weights * mean_y, axis=0, keepdims=True)
    proj_ref[...] = part_ref[...] - q * mixed_ref[...] - (local_cells * mean_y) * (q * mean_b + r)
    mean1 = spread_column(mean1, cols)
    scale1 = spread_column(scale1, cols)
    gain1 = spread_column(0.5 * gain1, cols)
    shift1 = spread_column(lift, cols)

    def narrow(j, carry):
        h = 2 * j
        lines = lane_pair(y_ref, h)
        back = nn_dot(mixer, jnp.concatenate([lines, lines], axis=0))
        for k in range(2):
            normed = (a_ref[h + k] - mean1) * scale1
            half = gain1 * normed + shift1
            t = jnp.tanh(half)
            slope = (0.5 + 0.5 * t) * (1.0 + half * (1.0 - t))
            grad = (f_ref[h + k] - back[:, k * cols : (k + 1) * cols] - level) * slope
            da_ref[h + k] = (back_front * (grad - flat - normed * tilt)).astype(bf16)
        return carry

    lax.fori_loop(0, rows // 2, narrow, 0, unroll=rows // 2)
    edge_pieces(
        lambda h: da_ref[h].astype(f32), rows, (depth, cols), row_ref, col_ref, corner_ref
    )


def corr_kernel(da_ref, shifted_ref, proj_ref, small_ref, out_ref, padded_ref):
    rows, depth, cols = da_ref.shape
    blank = jnp.zeros((2, depth, cols), bf16)
    padded_ref[pl.ds(0, 2)] = blank
    padded_ref[pl.ds(rows + 2, 2)] = blank

    def fill(h, carry):
        padded_ref[h + 2] = da_ref[h]
        return carry

    lax.fori_loop(0, rows, fill, 0, unroll=rows)
    tall = 3 * depth
    step = 6
    grad = jnp.zeros((tall, tall), f32)
    for start in range(0, rows + 2, step):
        lines = range(start, min(start + step, rows + 2))
        left = jnp.concatenate(
            [padded_ref[pl.ds(r, 3)].reshape(tall, cols) for r in lines], axis=1
        )
        right = jnp.concatenate([shifted_ref[r] for r in lines], axis=1)
        grad = grad + nt_dot(left, right)
    out_ref[0:tall] = grad[:, :128].astype(bf16)
    rest = grad[:, 128:]
    at = tall + tall // 2
    out_ref[tall:at] = jnp.concatenate([rest[: tall // 2], rest[tall // 2 :]], axis=1).astype(bf16)
    for k in range(0, proj_ref.shape[1], 128):
        out_ref[at : at + depth] = proj_ref[:, k : k + 128].astype(bf16)
        at += depth
    small = small_ref[...]
    high = small.astype(bf16).astype(f32)
    out_ref[at : at + 16] = jnp.concatenate([high, small - high], axis=0).astype(bf16)
    at += 16
    out_ref[at:] = jnp.zeros((out_ref.shape[0] - at, 128), bf16)


def beside_kernel(row_ref, col_ref, corner_ref, out_ref):
    out_ref[0] = row_ref[...]
    out_ref[1] = col_ref[...] + corner_ref[...]


def back_kernel(d_ref, beside_ref, w_ref, out_ref, shifted_ref):
    rows, _, _ = d_ref.shape
    border, side = beside_ref[0].astype(f32), beside_ref[1].astype(f32)
    three_shifts(lambda h: d_ref[h].astype(f32), border, side, shifted_ref)
    weights = w_ref[...]

    def body(j, carry):
        h = 4 * j
        for k, line in enumerate(conv_lines(weights, shifted_ref, h)):
            out_ref[h + k] = line.astype(bf16)
        return carry

    lax.fori_loop(0, rows // 4, body, 0, unroll=rows // 4)


def sum_kernel(parts_ref, out_ref):
    total = parts_ref[0].astype(f32)
    for d in range(1, parts_ref.shape[0]):
        total = total + parts_ref[d].astype(f32)
    total = total.astype(bf16)
    for d in range(parts_ref.shape[0]):
        out_ref[d] = total


def unpack_kernel(
    in_ref, conv_ref, proj_ref, gain1_ref, shift1_ref, gain3_ref, shift3_ref, *, factor
):
    depth, wide = proj_ref.shape
    tall = 3 * depth

    def take(start, stop):
        return in_ref[start:stop].astype(f32) * factor

    main = take(0, tall)
    at = tall + tall // 2
    rest = take(tall, at)
    rest = jnp.concatenate([rest[:, :depth], rest[:, depth:]], axis=0)
    for a in range(3):
        block = main[(2 - a) * depth : (3 - a) * depth]
        conv_ref[a, 0] = block[:, :depth]
        conv_ref[a, 1] = block[:, depth:]
        conv_ref[a, 2] = rest[(2 - a) * depth : (3 - a) * depth]
    for k in range(0, wide, 128):
        proj_ref[:, k : k + 128] = take(at, at + depth)
        at += depth
    both = take(at, at + 16)
    small = both[:8] + both[8:]
    shift1_ref[...] = small[0:1, :depth]
    gain1_ref[...] = small[0:1, depth : 2 * depth]
    steps = wide // 128
    for ref, start in ((shift3_ref, 1), (gain3_ref, 1 + steps)):
        for k in range(steps):
            ref[:, k * 128 : (k + 1) * 128] = small[start + k : start + k + 1]


def call(kernel, mib, outs, *args, scratch=()):
    return pl.pallas_call(
        kernel,
        out_shape=[jax.ShapeDtypeStruct(s, d) for s, d in outs],
        scratch_shapes=list(scratch),
        compiler_params=pltpu.CompilerParams(vmem_limit_bytes=mib * 1024 * 1024),
    )(*args)


def exchange(row, col, corner):
    return from_partner(row, 2), from_partner(col, 1), from_partner(corner, 3)


def swap(copies, axes):
    return lax.all_to_all(copies, axes, 0, 0)


def shards(
    images, out_grad, conv_weight, proj_weight, gain_one, shift_one, gain_three, shift_three
):
    depth, rows, cols = images.shape[2:]
    wide = out_grad.shape[2]
    group = lax.axis_size(group_axes)
    devices = lax.axis_size(all_axes)
    per_image = 1.0 / float(lax.axis_size("sp") * rows * cols)
    one = gain_one.reshape(1, -1), shift_one.reshape(1, -1)
    three = gain_three.reshape(1, -1), shift_three.reshape(1, -1)
    plane = (rows, depth, cols)
    piece = ((depth, cols), bf16)
    rows_out = ((group, 8, 128), f32)

    tall = pltpu.VMEM((depth * rows, cols), f32)
    keep = [pltpu.VMEM((4, wide, cols), f32)]
    lines, *edges = call(
        edge_kernel, EDGE, [(plane, bf16)] + [piece] * 3, images[0, 0], scratch=[tall]
    )
    (cotangent,) = call(
        lines_kernel, LINES, [((rows, wide, cols), bf16)], out_grad[0, 0], scratch=[tall]
    )
    ahead, behind, proj_t = call(
        weights_kernel, 4,
        [((2 * depth, 12 * depth), bf16)] * 2 + [((wide, depth), bf16)], conv_weight, proj_weight,
    )
    edges = exchange(*edges)
    triple = pltpu.VMEM((rows + 2, 3 * depth, cols), bf16)
    shifted, conv_out, stat = call(
        conv_kernel, CONV,
        [((rows + 2, 3 * depth, cols), bf16), (plane, f32), rows_out], lines, *edges, ahead,
    )
    stat_one = swap(stat, group_axes)
    hidden, turn, stat, mixed, mean_y = call(
        hidden_kernel, HIDDEN,
        [(plane, bf16), ((rows, 2 * depth, cols), bf16), ((group, 32 + depth, 128), bf16)]
        + [((depth, wide), f32), ((depth, cols), f32)],
        conv_out, stat_one, *one, proj_weight,
        scratch=[pltpu.VMEM(plane, bf16)],
    )
    stat_three = swap(stat, group_axes)
    narrowed, part, sums = call(
        slope_kernel, SLOPE, [(plane, f32), ((depth, wide), f32), rows_out],
        hidden, cotangent, turn, stat_three, *three, proj_t, proj_weight,
        scratch=keep + [pltpu.VMEM((rows, wide, cols), bf16)],
    )
    sums_three = swap(sums, group_axes)
    grad_conv, *last, proj, small = call(
        wide_kernel, WIDE,
        [(plane, bf16)] + [piece] * 3 + [((depth, wide), f32), ((8, 128), f32)],
        hidden, narrowed, conv_out, stat_one, *one, stat_three, three[0], sums_three,
        proj_weight, mixed, mean_y, part,
    )
    last = exchange(*last)
    used = 9 * depth * depth // 128 + depth * wide // 128 + 16
    used += -used % (16 * 32)
    (part,) = call(
        corr_kernel, GRAD, [((used, 128), bf16)], grad_conv, shifted, proj, small,
        scratch=[pltpu.VMEM((rows + 4, depth, cols), bf16)],
    )
    (last,) = call(beside_kernel, 1, [((2, depth, cols), bf16)], *last)
    (grad_field,) = call(
        back_kernel, BACK, [(plane, bf16)], grad_conv, last, behind, scratch=[triple]
    )
    part = jnp.pad(part, ((0, -used % (devices * 16)), (0, 0))).reshape(devices, -1, 128)
    parts = swap(part, all_axes)
    (mine,) = call(sum_kernel, 4, [(part.shape, bf16)], parts)
    full = swap(mine, all_axes)
    full = full.reshape(-1, 128)[:used]
    kernel_total, proj_total, gain1, shift1, gain3, shift3 = call(
        partial(unpack_kernel, factor=per_image), 4,
        [((3, 3, depth, depth), f32), ((depth, wide), f32)]
        + [((1, depth), f32)] * 2 + [((1, wide), f32)] * 2,
        full,
    )
    return (
        jnp.transpose(grad_field, (1, 0, 2))[None, None],
        kernel_total,
        proj_total,
        gain1[0],
        shift1[0],
        gain3[0],
        shift3[0],
    )


def solution(mesh):
    in_specs = (
        P(("bn", "dp"), "sp", None, None, None),
        P(("bn", "dp"), "sp", None, None, None),
        P(),
        P(),
        P(),
        P(),
        P(),
        P(),
    )
    out_specs = (P(("bn", "dp"), "sp", None, None, None), P(), P(), P(), P(), P(), P())
    return jax.shard_map(shards, mesh=mesh, in_specs=in_specs, out_specs=out_specs, check_vma=False)
```

```python
from functools import partial

import jax
import jax.numpy as jnp
from jax import lax
from jax.experimental import pallas as pl
from jax.experimental.pallas import tpu as pltpu
from jax.sharding import PartitionSpec as P


norm_floor = 1e-05
bf16 = jnp.bfloat16
f32 = jnp.float32
EDGE, LINES, CONV, HIDDEN, SLOPE, WIDE, GRAD, BACK = 8, 16, 14, 12, 24, 16, 16, 12
group_axes = ("sp", "bn")
all_axes = ("sp", "bn", "dp")


def from_partner(value, mask):
    return lax.ppermute(value, "sp", [(i, i ^ mask) for i in range(lax.axis_size("sp"))])


def nt_dot(left, right):
    return lax.dot_general(left, right, (((1,), (1,)), ((), ())), preferred_element_type=f32)


def nn_dot(left, right):
    return lax.dot_general(left, right, (((1,), (0,)), ((), ())), preferred_element_type=f32)


def lane_pair(ref, row):
    return jnp.concatenate([ref[row], ref[row + 1]], axis=1)


def row_of(partials):
    depth = partials.shape[0]
    if depth < 128:
        partials = jnp.concatenate([partials, jnp.zeros((128 - depth, 128), f32)], axis=0)
    pieces = [
        jnp.sum(jnp.transpose(partials[k : k + 128]), axis=0, keepdims=True)
        for k in range(0, partials.shape[0], 128)
    ]
    return pieces[0] if len(pieces) == 1 else jnp.concatenate(pieces, axis=1)


def columns_of(rows, depth):
    width = rows[0].shape[1]
    stacked = jnp.concatenate(rows + [jnp.zeros((128 - len(rows), width), f32)], axis=0)
    pieces = [jnp.transpose(stacked[:, k : k + 128]) for k in range(0, width, 128)]
    tall = pieces[0] if len(pieces) == 1 else jnp.concatenate(pieces, axis=0)
    return [tall[:depth, k : k + 1] for k in range(len(rows))]


def pack_rows(out_ref, rows):
    devices, height, width = out_ref.shape
    lines = [row[:, k : k + width] for row in rows for k in range(0, row.shape[1], width)]
    lines += [jnp.zeros((height - len(lines), width), f32)] if len(lines) < height else []
    block = jnp.concatenate(lines, axis=0)
    for d in range(devices):
        out_ref[d] = block


def device_rows(gathered_ref):
    blocks = []
    for d in range(gathered_ref.shape[0]):
        if gathered_ref.dtype == f32:
            blocks.append(gathered_ref[d, 0:8])
        else:
            parts = gathered_ref[d, 0:24].astype(f32)
            blocks.append(parts[0:8] + parts[8:16] + parts[16:24])
    return blocks


def row_at(block, kind, depth):
    steps = max(depth // 128, 1)
    lines = [block[k : k + 1] for k in range(kind * steps, (kind + 1) * steps)]
    return lines[0] if steps == 1 else jnp.concatenate(lines, axis=1)


def joined_moments(gathered_ref, local_cells, depth):
    blocks = device_rows(gathered_ref)
    devices = len(blocks)
    means = [row_at(block, 0, depth) for block in blocks]
    average = sum(means[1:], means[0]) * (1.0 / devices)
    squares = None
    for block, mean in zip(blocks, means):
        delta = mean - average
        term = row_at(block, 1, depth) + local_cells * (delta * delta)
        squares = term if squares is None else squares + term
    return average, squares * (1.0 / (devices * local_cells))


def summed_block(gathered_ref):
    blocks = device_rows(gathered_ref)
    return sum(blocks[1:], blocks[0])


def place_flags():
    position = lax.axis_index("sp")
    return position % 2, position // 2


def edge_pieces(line_of, rows, shape, row_ref, col_ref, corner_ref, at=0):
    depth, cols = shape
    column, half = place_flags()
    lane = lax.broadcasted_iota(jnp.int32, (depth, cols), 1)
    edge = jnp.where(column == 0, cols - 1, 0)

    def body(h, found):
        moved = pltpu.roll(line_of(h), lax.rem(h + 1 - edge + cols, cols), 1)
        return jnp.where(lane == h + 1, moved, found)

    kind = row_ref.dtype
    block = pl.ds(at, depth)
    found = lax.fori_loop(0, rows, body, jnp.zeros((depth, cols), f32), unroll=rows)
    col_ref[block] = found.astype(kind)
    border = line_of(jnp.where(half == 0, rows - 1, 0))
    row_ref[block] = border.astype(kind)
    target = jnp.where(half == 0, 0, rows + 1)
    moved = pltpu.roll(border, lax.rem(target - edge + cols, cols), 1)
    corner_ref[block] = jnp.where(lane == target, moved, 0.0).astype(kind)


def three_shifts(line_of, border, side, out_ref):
    rows = out_ref.shape[0] - 2
    depth, cols = border.shape
    column, half = place_flags()
    lane = lax.broadcasted_iota(jnp.int32, (depth, cols), 1)
    start = jnp.where(column == 1, cols, 2 * cols - 1)

    def place(r, line):
        before = pltpu.roll(line, 1, 1)
        after = pltpu.roll(line, cols - 1, 1)
        edge = pltpu.roll(side, lax.rem(start - r, cols), 1)
        before = jnp.where(lane == 0, jnp.where(column == 1, edge, 0.0), before)
        after = jnp.where(lane == cols - 1, jnp.where(column == 0, edge, 0.0), after)
        out_ref[r] = jnp.concatenate([before, line, after], axis=0).astype(bf16)

    place(0, jnp.where(half == 1, border, 0.0))
    place(rows + 1, jnp.where(half == 0, border, 0.0))

    def body(h, carry):
        place(h + 1, line_of(h))
        return carry

    lax.fori_loop(0, rows, body, 0, unroll=rows)


def conv_lines(weights, shifted_ref, row):
    depth3 = shifted_ref.shape[1]
    cols = shifted_ref.shape[2]
    depth = depth3 // 3
    first = shifted_ref[pl.ds(row, 4)].reshape(4 * depth3, cols)
    second = shifted_ref[pl.ds(row + 2, 4)].reshape(4 * depth3, cols)
    found = nn_dot(weights, jnp.concatenate([first, second], axis=1))
    return [
        found[u * depth : (u + 1) * depth, k * cols : (k + 1) * cols]
        for k in range(2)
        for u in range(2)
    ]


def to_lines(planes_ref, out_ref, tall_ref):
    depth, rows, _ = planes_ref.shape
    block = tall_ref.shape[0] // rows
    for start in range(0, depth, block):

        def spill(c, carry, start=start):
            at = pl.multiple_of(c * rows, 8)
            tall_ref[pl.ds(at, rows), :] = planes_ref[start + c].astype(f32)
            return carry

        lax.fori_loop(0, block, spill, 0, unroll=block)

        def collect(h, carry, start=start):
            line = tall_ref[pl.ds(h, block, stride=rows), :]
            out_ref[h, start : start + block] = line.astype(bf16)
            return carry

        lax.fori_loop(0, rows, collect, 0, unroll=rows)


def edge_kernel(planes_ref, lines_ref, row_ref, col_ref, corner_ref, tall_ref):
    rows, depth, cols = lines_ref.shape
    to_lines(planes_ref, lines_ref, tall_ref)
    edge_pieces(
        lambda h: lines_ref[h].astype(f32), rows, (depth, cols), row_ref, col_ref, corner_ref
    )


def lines_kernel(planes_ref, lines_ref, tall_ref):
    to_lines(planes_ref, lines_ref, tall_ref)


def weights_kernel(conv_ref, proj_ref, ahead_ref, behind_ref, across_ref):
    depth, wide = proj_ref.shape
    blank = jnp.zeros((depth, 128 - depth), f32)

    def turned(block):
        block = jnp.concatenate([block, blank], axis=1) if depth < 128 else block
        tall = jnp.zeros((128 - depth, 128), f32)
        block = jnp.concatenate([block, tall], axis=0) if depth < 128 else block
        return jnp.transpose(block)[:depth, :depth]

    forth, back = [], []
    for a in range(3):
        for b in range(3):
            forth.append(conv_ref[a, b])
            back.append(turned(conv_ref[2 - a, 2 - b].astype(f32)).astype(bf16))
    gap = [jnp.zeros((depth, depth), bf16)] * 3
    for ref, blocks in ((ahead_ref, forth), (behind_ref, back)):
        ref[:depth] = jnp.concatenate(blocks + gap, axis=1)
        ref[depth:] = jnp.concatenate(gap + blocks, axis=1)
    for k in range(0, wide, 128):
        block = proj_ref[:, k : k + 128].astype(f32)
        block = jnp.concatenate([block, jnp.zeros((128 - depth, 128), f32)], axis=0)
        across_ref[k : k + 128] = jnp.transpose(block)[:, :depth].astype(bf16)


def conv_kernel(x_ref, row_ref, col_ref, corner_ref, w_ref, shifted_ref, a_ref, stat_ref):
    rows, depth, cols = x_ref.shape
    side = col_ref[...].astype(f32) + corner_ref[...].astype(f32)
    three_shifts(lambda h: x_ref[h].astype(f32), row_ref[...].astype(f32), side, shifted_ref)
    weights = w_ref[...]

    def body(j, total):
        h = 4 * j
        for k, line in enumerate(conv_lines(weights, shifted_ref, h)):
            a_ref[h + k] = line
            total = total + line
        return total

    total = lax.fori_loop(0, rows // 4, body, jnp.zeros((depth, cols), f32), unroll=rows // 4)
    mean = jnp.sum(total, axis=1, keepdims=True) * (1.0 / (rows * cols))

    def spread(h, squares):
        centred = a_ref[h] - mean
        return squares + centred * centred

    squares = lax.fori_loop(0, rows, spread, jnp.zeros((depth, cols), f32), unroll=rows)
    pack_rows(stat_ref, [row_of(total) * (1.0 / (rows * cols)), row_of(squares)])


def wide_row(ref):
    row = ref[...]
    short = -row.shape[1] % 128
    return jnp.concatenate([row, jnp.zeros((1, short), f32)], axis=1) if short else row


def norm_columns(gathered_ref, gain_ref, shift_ref, local_cells):
    depth = gain_ref.shape[1]
    average, variance = joined_moments(gathered_ref, local_cells, depth)
    scale = lax.rsqrt(variance + norm_floor)
    return columns_of([average, scale, wide_row(gain_ref), wide_row(shift_ref)], depth)


def spread_column(column, cols):
    return jnp.broadcast_to(column, (column.shape[0], cols))


def hidden_kernel(
    a_ref, stat_ref, gain_ref, shift_ref, w_ref,
    y_ref, turn_ref, out_ref, mixed_ref, mean_ref, centred_ref,
):
    rows, depth, cols = a_ref.shape
    cells = float(rows * cols)
    mean, scale, gain, shift = norm_columns(stat_ref, gain_ref, shift_ref, cells)
    gain = spread_column(0.5 * gain, cols)
    scale = spread_column(scale, cols)
    mean = spread_column(mean, cols)
    lift = spread_column(0.5 * shift, cols)
    rest = jnp.tanh(lift)
    middle = (lift + lift * rest).astype(bf16).astype(f32)
    level = (0.5 + 0.5 * rest) * (1.0 + lift * (1.0 - rest))

    def activate(h, carry):
        total, turned = carry
        normed = (a_ref[h] - mean) * scale
        half = normed * gain + lift
        t = jnp.tanh(half)
        hidden = (half + half * t).astype(bf16)
        slope = (0.5 + 0.5 * t) * (1.0 + half * (1.0 - t))
        turn = jnp.concatenate([slope - level, slope * normed], axis=0)
        turn_ref[h] = turn.astype(bf16)
        y_ref[h] = hidden
        centred = hidden.astype(f32) - middle
        centred_ref[h] = centred.astype(bf16)
        return total + centred, turned + turn

    zero = jnp.zeros((depth, cols), f32)
    both = jnp.zeros((2 * depth, cols), f32)
    total, turned = lax.fori_loop(0, rows, activate, (zero, both), unroll=rows)
    gram = jnp.zeros((depth, 3 * depth), f32)
    step = rows
    for h in range(0, rows, step):
        lines = range(h, min(h + step, rows))
        left = jnp.concatenate([centred_ref[k] for k in lines], axis=1)
        right = jnp.concatenate([turn_ref[k] for k in lines], axis=1)
        gram = gram + nt_dot(left, jnp.concatenate([right, left], axis=0))
    across = gram[:, : 2 * depth]
    gram = gram[:, 2 * depth :]
    weights = w_ref[...].astype(f32)
    mean_c = jnp.sum(total, axis=1, keepdims=True) * (1.0 / cells)
    mean_r = row_of(total)[:, :depth] * (1.0 / cells)
    spread = gram - cells * (mean_c * mean_r)
    mixed = lax.dot_general(
        spread, weights, (((1,), (0,)), ((), ())),
        precision=lax.Precision.HIGHEST, preferred_element_type=f32,
    )
    mixed_ref[...] = mixed
    mean_ref[...] = mean_c + middle
    squares = jnp.maximum(jnp.sum(mixed * weights, axis=0, keepdims=True), 0.0)
    means = jnp.sum(weights * (mean_c + middle[:, 0:1]), axis=0, keepdims=True)
    width = out_ref.shape[2]
    lines = [row[:, k : k + width] for row in (means, squares) for k in range(0, row.shape[1], width)]
    lines.append(row_of(turned))
    block = jnp.concatenate(lines + [jnp.zeros((8 - len(lines), width), f32)], axis=0)
    high = block.astype(bf16).astype(f32)
    middle = (block - high).astype(bf16).astype(f32)
    low = block - high - middle
    block = jnp.concatenate([high, middle, low, across], axis=0)
    block = block.astype(bf16)
    for d in range(out_ref.shape[0]):
        out_ref[d] = block


def slope_kernel(
    y_ref, g_ref, turn_ref, stat_ref, gain_ref, shift_ref, w_ref, wt_ref,
    f_ref, proj_ref, out_ref, keep_ref, e_ref,
):
    rows, depth, cols = y_ref.shape
    wide = w_ref.shape[0]
    mean, scale, gain, shift = norm_columns(stat_ref, gain_ref, shift_ref, float(rows * cols))
    steep = 0.5 * gain * scale
    keep_ref[0] = spread_column(steep, cols)
    keep_ref[1] = spread_column(0.5 * shift - mean * steep, cols)
    keep_ref[2] = jnp.zeros((wide, cols), f32)
    keep_ref[3] = jnp.zeros((wide, cols), f32)
    proj_ref[...] = jnp.zeros(proj_ref.shape, f32)
    block = 64
    weights_t = wt_ref[...]

    def expand(j):
        h = 2 * j
        lines = lane_pair(y_ref, h)
        for start in range(0, wide, block):
            part = slice(start, start + block)
            both = nn_dot(w_ref[part], lines)
            s, b = keep_ref[0, part], keep_ref[1, part]
            total = cross = None
            for k in range(2):
                half = both[:, k * cols : (k + 1) * cols] * s + b
                t = jnp.tanh(half)
                slope = (1.0 + t) * (1.0 + half * (1.0 - t))
                grad = g_ref[h + k, part].astype(f32) * slope
                e_ref[h + k, part] = (grad * s).astype(bf16)
                across = grad * half
                total = grad if total is None else total + grad
                cross = across if cross is None else cross + across
            keep_ref[2, part] += total
            keep_ref[3, part] += cross

    def narrow(j, turned):
        h = 2 * j
        scaled = lane_pair(e_ref, h)
        both = nn_dot(weights_t, scaled)
        proj_ref[...] += nt_dot(lane_pair(y_ref, h), scaled)
        for k in range(2):
            line = both[:, k * cols : (k + 1) * cols]
            f_ref[h + k] = line
            turned = turned + jnp.concatenate([line, line], axis=0) * turn_ref[h + k].astype(f32)
        return turned

    def body(j, turned):
        expand(j)
        turned = narrow(j - 1, turned)
        return turned

    expand(0)
    turned = jnp.zeros((2 * depth, cols), f32)
    turned = lax.fori_loop(1, rows // 2, body, turned, unroll=rows // 2 - 1)
    turned = narrow(rows // 2 - 1, turned)
    total = row_of(keep_ref[2]) * 0.5
    cross = row_of(keep_ref[3])
    cross = (cross - shift_ref[...] * total) / gain_ref[...]
    pack_rows(out_ref, [total, cross, row_of(turned)])


def wide_kernel(
    y_ref, f_ref, a_ref, stat1_ref, gain1_ref, shift1_ref, stat3_ref, gain3_ref, sums_ref,
    wt_ref, mixed_ref, mean_ref, part_ref,
    da_ref, row_ref, col_ref, corner_ref, proj_ref, small_ref,
):
    rows, depth, cols = y_ref.shape
    wide = wt_ref.shape[1]
    local_cells = float(rows * cols)
    devices = sums_ref.shape[0]
    cells = local_cells * devices
    mean3, variance3 = joined_moments(stat3_ref, local_cells, wide)
    scale3 = lax.rsqrt(variance3 + norm_floor)
    front = gain3_ref[...] * scale3
    sums = summed_block(sums_ref)
    steps = wide // 128
    q = front * scale3 * row_at(sums, 1, wide) * (1.0 / cells)
    r = front * row_at(sums, 0, wide) * (1.0 / cells) - q * mean3
    weights = wt_ref[...].astype(f32)
    exact = lax.Precision.HIGHEST
    mixer = lax.dot_general(
        weights * q, weights, (((1,), (1,)), ((), ())),
        precision=exact, preferred_element_type=f32,
    )
    level_row = lax.dot_general(
        jnp.broadcast_to(r, (8, wide)), weights, (((1,), (1,)), ((), ())),
        precision=exact, preferred_element_type=f32,
    )[0:1]
    mean1, scale1, gain1, shift1 = norm_columns(stat1_ref, gain1_ref, shift1_ref, local_cells)
    lift = 0.5 * shift1
    middle = (lift + lift * jnp.tanh(lift)).astype(bf16).astype(f32)
    level_row = level_row + jnp.sum(mixer * middle, axis=0, keepdims=True)
    across = stat3_ref[0, 24 : 24 + depth].astype(f32)
    for d in range(1, devices):
        across = across + stat3_ref[d, 24 : 24 + depth].astype(f32)
    turned = summed_block(stat3_ref)[2 * steps : 2 * steps + 1]
    double = jnp.concatenate([mixer, mixer], axis=1)
    sums_one = sums[2 * steps : 2 * steps + 1] - jnp.sum(double * across, axis=0, keepdims=True)
    sums_one = sums_one - jnp.concatenate([level_row, level_row], axis=1) * turned
    blank = jnp.zeros((8 - 1 - 2 * steps, 128), f32)
    small_ref[...] = jnp.concatenate([sums_one, sums[: 2 * steps], blank], axis=0) * (1.0 / devices)
    (column,) = columns_of([sums_one], 2 * depth)
    back_front = spread_column(gain1 * scale1, cols)
    flat = spread_column(column[:depth] * (1.0 / cells), cols)
    tilt = spread_column(column[depth:] * (1.0 / cells), cols)
    mixer_high = mixer.astype(bf16)
    mixer = jnp.concatenate([mixer_high, (mixer - mixer_high.astype(f32)).astype(bf16)], axis=1)
    level = spread_column(jnp.sum(weights * r, axis=1, keepdims=True), cols)
    mean_y = mean_ref[:, 0:1]
    mean_b = jnp.sum(weights * mean_y, axis=0, keepdims=True)
    proj_ref[...] = part_ref[...] - q * mixed_ref[...] - (local_cells * mean_y) * (q * mean_b + r)
    mean1 = spread_column(mean1, cols)
    scale1 = spread_column(scale1, cols)
    gain1 = spread_column(0.5 * gain1, cols)
    shift1 = spread_column(lift, cols)

    def narrow(j, carry):
        h = 2 * j
        lines = lane_pair(y_ref, h)
        back = nn_dot(mixer, jnp.concatenate([lines, lines], axis=0))
        for k in range(2):
            normed = (a_ref[h + k] - mean1) * scale1
            half = gain1 * normed + shift1
            t = jnp.tanh(half)
            slope = (0.5 + 0.5 * t) * (1.0 + half * (1.0 - t))
            grad = (f_ref[h + k] - back[:, k * cols : (k + 1) * cols] - level) * slope
            da_ref[h + k] = (back_front * (grad - flat - normed * tilt)).astype(bf16)
        return carry

    lax.fori_loop(0, rows // 2, narrow, 0, unroll=rows // 2)
    edge_pieces(
        lambda h: da_ref[h].astype(f32), rows, (depth, cols), row_ref, col_ref, corner_ref
    )


def corr_kernel(da_ref, shifted_ref, proj_ref, small_ref, out_ref, padded_ref):
    rows, depth, cols = da_ref.shape
    blank = jnp.zeros((2, depth, cols), bf16)
    padded_ref[pl.ds(0, 2)] = blank
    padded_ref[pl.ds(rows + 2, 2)] = blank

    def fill(h, carry):
        padded_ref[h + 2] = da_ref[h]
        return carry

    lax.fori_loop(0, rows, fill, 0, unroll=rows)
    tall = 3 * depth
    step = rows + 2
    grad = jnp.zeros((tall, tall), f32)
    for start in range(0, rows + 2, step):
        lines = range(start, min(start + step, rows + 2))
        left = jnp.concatenate(
            [padded_ref[pl.ds(r, 3)].reshape(tall, cols) for r in lines], axis=1
        )
        right = jnp.concatenate([shifted_ref[r] for r in lines], axis=1)
        grad = grad + nt_dot(left, right)
    out_ref[0:tall] = grad[:, :128].astype(bf16)
    rest = grad[:, 128:]
    at = tall + tall // 2
    out_ref[tall:at] = jnp.concatenate([rest[: tall // 2], rest[tall // 2 :]], axis=1).astype(bf16)
    for k in range(0, proj_ref.shape[1], 128):
        out_ref[at : at + depth] = proj_ref[:, k : k + 128].astype(bf16)
        at += depth
    small = small_ref[...]
    high = small.astype(bf16).astype(f32)
    out_ref[at : at + 16] = jnp.concatenate([high, small - high], axis=0).astype(bf16)
    at += 16
    out_ref[at:] = jnp.zeros((out_ref.shape[0] - at, 128), bf16)


def beside_kernel(row_ref, col_ref, corner_ref, out_ref):
    out_ref[0] = row_ref[...]
    out_ref[1] = col_ref[...] + corner_ref[...]


def back_kernel(d_ref, beside_ref, w_ref, out_ref, shifted_ref):
    rows, _, _ = d_ref.shape
    border, side = beside_ref[0].astype(f32), beside_ref[1].astype(f32)
    three_shifts(lambda h: d_ref[h].astype(f32), border, side, shifted_ref)
    weights = w_ref[...]

    def body(j, carry):
        h = 4 * j
        for k, line in enumerate(conv_lines(weights, shifted_ref, h)):
            out_ref[h + k] = line.astype(bf16)
        return carry

    lax.fori_loop(0, rows // 4, body, 0, unroll=rows // 4)


def sum_kernel(parts_ref, out_ref):
    total = parts_ref[0].astype(f32)
    for d in range(1, parts_ref.shape[0]):
        total = total + parts_ref[d].astype(f32)
    total = total.astype(bf16)
    for d in range(parts_ref.shape[0]):
        out_ref[d] = total


def unpack_kernel(
    in_ref, conv_ref, proj_ref, gain1_ref, shift1_ref, gain3_ref, shift3_ref, *, factor
):
    depth, wide = proj_ref.shape
    tall = 3 * depth

    def take(start, stop):
        return in_ref[start:stop].astype(f32) * factor

    main = take(0, tall)
    at = tall + tall // 2
    rest = take(tall, at)
    rest = jnp.concatenate([rest[:, :depth], rest[:, depth:]], axis=0)
    for a in range(3):
        block = main[(2 - a) * depth : (3 - a) * depth]
        conv_ref[a, 0] = block[:, :depth]
        conv_ref[a, 1] = block[:, depth:]
        conv_ref[a, 2] = rest[(2 - a) * depth : (3 - a) * depth]
    for k in range(0, wide, 128):
        proj_ref[:, k : k + 128] = take(at, at + depth)
        at += depth
    both = take(at, at + 16)
    small = both[:8] + both[8:]
    shift1_ref[...] = small[0:1, :depth]
    gain1_ref[...] = small[0:1, depth : 2 * depth]
    steps = wide // 128
    for ref, start in ((shift3_ref, 1), (gain3_ref, 1 + steps)):
        for k in range(steps):
            ref[:, k * 128 : (k + 1) * 128] = small[start + k : start + k + 1]


def call(kernel, mib, outs, *args, scratch=()):
    return pl.pallas_call(
        kernel,
        out_shape=[jax.ShapeDtypeStruct(s, d) for s, d in outs],
        scratch_shapes=list(scratch),
        compiler_params=pltpu.CompilerParams(vmem_limit_bytes=mib * 1024 * 1024),
    )(*args)


def exchange(row, col, corner):
    return from_partner(row, 2), from_partner(col, 1), from_partner(corner, 3)


def swap(copies, axes):
    return lax.all_to_all(copies, axes, 0, 0)


def shards(
    images, out_grad, conv_weight, proj_weight, gain_one, shift_one, gain_three, shift_three
):
    depth, rows, cols = images.shape[2:]
    wide = out_grad.shape[2]
    group = lax.axis_size(group_axes)
    devices = lax.axis_size(all_axes)
    per_image = 1.0 / float(lax.axis_size("sp") * rows * cols)
    one = gain_one.reshape(1, -1), shift_one.reshape(1, -1)
    three = gain_three.reshape(1, -1), shift_three.reshape(1, -1)
    plane = (rows, depth, cols)
    piece = ((depth, cols), bf16)
    rows_out = ((group, 8, 128), f32)

    tall = pltpu.VMEM((depth * rows, cols), f32)
    keep = [pltpu.VMEM((4, wide, cols), f32)]
    lines, *edges = call(
        edge_kernel, EDGE, [(plane, bf16)] + [piece] * 3, images[0, 0], scratch=[tall]
    )
    (cotangent,) = call(
        lines_kernel, LINES, [((rows, wide, cols), bf16)], out_grad[0, 0], scratch=[tall]
    )
    ahead, behind, proj_t = call(
        weights_kernel, 4,
        [((2 * depth, 12 * depth), bf16)] * 2 + [((wide, depth), bf16)], conv_weight, proj_weight,
    )
    edges = exchange(*edges)
    triple = pltpu.VMEM((rows + 2, 3 * depth, cols), bf16)
    shifted, conv_out, stat = call(
        conv_kernel, CONV,
        [((rows + 2, 3 * depth, cols), bf16), (plane, f32), rows_out], lines, *edges, ahead,
    )
    stat_one = swap(stat, group_axes)
    hidden, turn, stat, mixed, mean_y = call(
        hidden_kernel, HIDDEN,
        [(plane, bf16), ((rows, 2 * depth, cols), bf16), ((group, 24 + depth, 128), bf16)]
        + [((depth, wide), f32), ((depth, cols), f32)],
        conv_out, stat_one, *one, proj_weight,
        scratch=[pltpu.VMEM(plane, bf16)],
    )
    stat_three = swap(stat, group_axes)
    narrowed, part, sums = call(
        slope_kernel, SLOPE, [(plane, f32), ((depth, wide), f32), rows_out],
        hidden, cotangent, turn, stat_three, *three, proj_t, proj_weight,
        scratch=keep + [pltpu.VMEM((rows, wide, cols), bf16)],
    )
    sums_three = swap(sums, group_axes)
    grad_conv, *last, proj, small = call(
        wide_kernel, WIDE,
        [(plane, bf16)] + [piece] * 3 + [((depth, wide), f32), ((8, 128), f32)],
        hidden, narrowed, conv_out, stat_one, *one, stat_three, three[0], sums_three,
        proj_weight, mixed, mean_y, part,
    )
    last = exchange(*last)
    used = 9 * depth * depth // 128 + depth * wide // 128 + 16
    used += -used % (16 * 32)
    (part,) = call(
        corr_kernel, GRAD, [((used, 128), bf16)], grad_conv, shifted, proj, small,
        scratch=[pltpu.VMEM((rows + 4, depth, cols), bf16)],
    )
    (last,) = call(beside_kernel, 1, [((2, depth, cols), bf16)], *last)
    (grad_field,) = call(
        back_kernel, BACK, [(plane, bf16)], grad_conv, last, behind, scratch=[triple]
    )
    part = jnp.pad(part, ((0, -used % (devices * 16)), (0, 0))).reshape(devices, -1, 128)
    parts = swap(part, all_axes)
    (mine,) = call(sum_kernel, 4, [(part.shape, bf16)], parts)
    full = swap(mine, all_axes)
    full = full.reshape(-1, 128)[:used]
    kernel_total, proj_total, gain1, shift1, gain3, shift3 = call(
        partial(unpack_kernel, factor=per_image), 4,
        [((3, 3, depth, depth), f32), ((depth, wide), f32)]
        + [((1, depth), f32)] * 2 + [((1, wide), f32)] * 2,
        full,
    )
    return (
        jnp.transpose(grad_field, (1, 0, 2))[None, None],
        kernel_total,
        proj_total,
        gain1[0],
        shift1[0],
        gain3[0],
        shift3[0],
    )


def solution(mesh):
    in_specs = (
        P(("bn", "dp"), "sp", None, None, None),
        P(("bn", "dp"), "sp", None, None, None),
        P(),
        P(),
        P(),
        P(),
        P(),
        P(),
    )
    out_specs = (P(("bn", "dp"), "sp", None, None, None), P(), P(), P(), P(), P(), P())
    return jax.shard_map(shards, mesh=mesh, in_specs=in_specs, out_specs=out_specs, check_vma=False)
```
